32 devices in a mesh: grp: 4 (over y, x), col: 8 (over z, core).
Axes of the slice: x: 2, y: 2, z: 4, core: 2. Of those that a mesh axis runs over, the one named last changes fastest.
Arguments:
- panels: bfloat16 [32, 4, 512, 512], P('col', None, 'grp'), may hold values from -1.296875 to 1.296875
- parent: float32 [32, 512, 512], P('col', 'grp'), may hold values from -6 to 6
- src_block: int32 [8, 40], P('col'), may hold values from 0 to 39, each once within a row
- dest_owner: int32 [320, 1], P('col'), may hold values from 0 to 7; in each aligned block of 40 rows (0 to 39, 40 to 79, ...) at most 7 rows name the same one
- target: int32 [320], P('col'), may hold values from 0 to 3
- counts: int32 [8], P('col'), may hold values from 20 to 40, as said below
Outputs:
- assembled: float32 [32, 512, 512], P('col', 'grp')
The draws below stay inside these ranges and needn't reach their ends.
Inputs may be any that keep to these rules, and one draw needn't show every extreme that they name: `src_block`: each row of a column rank is a permutation of the 40 block pairs. `dest_owner`: among the 40 slots of one column rank at most 7 name the same owner. The live slots of a rank are its first counts[c]; some rank has all 40 live.
All inputs are finite; a program needn't handle non-finite values.
Results may differ from the reference program's by a relative error of at most 0.0026.
Values may be sent and summed in bfloat16 or wider, within the bound.
A program may use at most 128 MiB of HBM per device.

```python
import math
import jax
import jax.numpy as jnp
import numpy as np
from jax import lax

WIDTH = 512
BLOCK = 512
ROW_BLOCKS = 4
FRONTS = 4
TARGETS = 4
PAIRS = 10
SLOTS = 40
CAPACITY = 7
N_COL = 8


def draw_counts(key, part):
    values = jax.random.randint(key, (N_COL,), SLOTS // 2, SLOTS + 1).astype(jnp.int32)
    chosen = jax.random.randint(jax.random.fold_in(key, 7), (), 0, N_COL)
    return values.at[chosen].set(SLOTS)


def set_ends(drawn, own_key, least, high):
    index_at = [jax.random.randint(jax.random.fold_in(own_key, axis), (), 0, length) for axis, length in enumerate(drawn.shape)]
    widest = drawn.shape.index(max(drawn.shape))
    next_to = index_at[:widest] + [(index_at[widest] + 1) % drawn.shape[widest]] + index_at[widest + 1:]
    return drawn.at[tuple(index_at)].set(least).at[tuple(next_to)].set(high)


def level_of(stream_key, shape, cuts, low, top_value):
    def one(position, shards_of):
        steps = jax.random.uniform(jax.random.fold_in(jax.random.fold_in(stream_key, 6), position), (shards_of,), jnp.float32, low / len(cuts), top_value / len(cuts))
        return jnp.repeat(jnp.exp(steps), shape[position] // shards_of).reshape((-1,) + (1,) * (len(shape) - position - 1))

    factor_of = one(*cuts[0])
    for cut in cuts[1:]:
        factor_of = factor_of * one(*cut)
    return factor_of


def shared_out(stream_key, own, number, rows, amount, top, bound, slope):
    ranking = jax.random.permutation(stream_key, amount)
    crowded, common = load_shares(amount, rows * top, bound, slope, True), load_shares(amount, rows * top, bound, slope, False)
    places = jnp.arange(amount)

    def named(lengths, turn):
        used = int((lengths > 0).sum())
        fixed = max(1, used // 4)
        passed = fixed + (places - fixed + turn * (used - fixed)) % max(1, amount - fixed)
        return jnp.zeros((amount,), jnp.int32).at[ranking[jnp.where(places < fixed, places, passed)]].set(jnp.asarray(lengths, jnp.int32))

    lengths = jnp.where(number % 4 == 0, named(crowded, number // 4), named(common, number - number // 4 - 1))
    mixed = jax.random.permutation(jax.random.fold_in(own, 3), amount)
    giver, sink = mixed[0:amount // 2 * 2:2], mixed[1:amount // 2 * 2:2]
    slack = jnp.minimum(lengths[giver] - 1, bound - lengths[sink]) // 2
    slack = jnp.where((giver == ranking[0]) | (sink == ranking[0]) | (lengths[sink] == 0), 0, jnp.maximum(slack, 0))
    passed = jax.random.randint(jax.random.fold_in(own, 4), (amount // 2,), 0, 1 << 20) % (slack + 1)
    lengths = lengths.at[giver].add(-passed).at[sink].add(passed)
    members = jnp.searchsorted(jnp.cumsum(lengths), jnp.arange(rows * top), side="right").astype(jnp.int32)
    listing = members.reshape(top, rows).T
    listing = listing[jax.random.permutation(jax.random.fold_in(own, 1), rows)]
    turn = jax.random.randint(jax.random.fold_in(own, 2), (rows, 1), 0, top)
    return jnp.take_along_axis(listing, (jnp.arange(top)[None, :] + turn) % top, axis=1)


def load_shares(amount, total, most, skew, full):
    portions = [(1 << 20) // math.isqrt(rank ** skew) + 1 for rank in range(1, amount + 1)]
    largest = most if full else min(most, max(-(-total // amount), total * portions[0] // sum(portions)))
    least = 1 if total - largest >= amount - 1 else 0
    given, rest = [largest] + [least] * (amount - 1), total - largest - least * (amount - 1)
    while rest > 0:
        candidates = [i for i in range(1, amount) if given[i] < largest] or [i for i in range(1, amount) if given[i] < most]
        whole, remaining = sum([portions[i] for i in candidates]), rest
        for i in candidates:
            addition = min(most - given[i], max(1, remaining * portions[i] // whole), rest)
            given[i] = given[i] + addition
            rest = rest - addition
    return np.array(given)


def centred(stream_key, shape, spread, most, shards=(), kind=jnp.bfloat16):
    result = jax.random.normal(stream_key, shape, jnp.float32) * spread
    if len(shards) > 0:
        result = level_of(stream_key, shape, shards, -0.22, 0.18) * result
    return jnp.clip(result, min=-most, max=most).astype(kind)


def setup_inputs(seed: int = 0) -> dict:
    streams_of = jax.random.split(jax.random.key(seed), 7)
    panels = centred(streams_of[0], (N_COL * FRONTS, ROW_BLOCKS, BLOCK, WIDTH), 0.21, 1.296875, ((0, 8), (2, 4)))
    parent = centred(streams_of[1], (N_COL * TARGETS, BLOCK, BLOCK), 1.0, 6.0, ((0, 8), (1, 4)), jnp.float32)
    src_block = jax.vmap(lambda own: jax.random.permutation(own, SLOTS))(jax.random.split(streams_of[2], N_COL)).reshape((N_COL, SLOTS)).astype(jnp.int32)
    dest_owner_keys = jax.random.split(jax.random.fold_in(streams_of[3], 1), (N_COL * SLOTS) // SLOTS)
    dest_owner_turns = jax.random.permutation(jax.random.fold_in(streams_of[3], 3), (N_COL * SLOTS) // SLOTS)
    dest_owner = jax.vmap(lambda own, number: shared_out(jax.random.fold_in(streams_of[3], 2), own, number, SLOTS, N_COL, 1, CAPACITY, 2))(dest_owner_keys, dest_owner_turns).reshape((N_COL * SLOTS, 1))
    target = set_ends(jax.random.randint(streams_of[4], (N_COL * SLOTS,), 0, TARGETS), jax.random.fold_in(streams_of[4], 1), 0, TARGETS - 1).astype(jnp.int32)
    counts = draw_counts(jax.random.fold_in(streams_of[6], 71), 0)
    return dict(panels=panels, parent=parent, src_block=src_block, dest_owner=dest_owner, target=target, counts=counts)


def reference(panels, parent, src_block, dest_owner, target, counts):
    running = parent.astype(jnp.float32)
    slot_index = jnp.arange(SLOTS, dtype=jnp.int32)
    upper_table = jnp.asarray(np.array([a for a in range(ROW_BLOCKS) for b in range(a + 1)], np.int32))
    lower_table = jnp.asarray(np.array([b for a in range(ROW_BLOCKS) for b in range(a + 1)], np.int32))

    def add_device(column_rank, running):
        own_panels = lax.dynamic_slice_in_dim(panels, (column_rank * FRONTS).astype(jnp.int32), FRONTS, 0)
        flat_rows = own_panels.astype(jnp.float32).reshape(FRONTS * ROW_BLOCKS, BLOCK, WIDTH)
        combos = lax.dynamic_index_in_dim(src_block, column_rank, 0, keepdims=False)
        front_of = combos // PAIRS
        within = combos % PAIRS
        left_index = (front_of * ROW_BLOCKS + upper_table[within]).astype(jnp.int32)
        right_index = (front_of * ROW_BLOCKS + lower_table[within]).astype(jnp.int32)
        left_rows = flat_rows[left_index]
        right_rows = flat_rows[right_index]
        updates = jnp.einsum("srw,scw->src", left_rows, right_rows, precision=lax.Precision.HIGHEST)
        updates = updates.astype(jnp.bfloat16).astype(jnp.float32)
        limit = lax.dynamic_index_in_dim(counts, column_rank, 0, keepdims=False)
        is_live = slot_index < limit
        updates = jnp.where(is_live[:, None, None], updates, jnp.zeros_like(updates))
        start = (column_rank * SLOTS).astype(jnp.int32)
        owner_rank = lax.dynamic_slice_in_dim(dest_owner[:, 0], start, SLOTS, 0)
        block_target = lax.dynamic_slice_in_dim(target, start, SLOTS, 0)
        dest_rows = (owner_rank * TARGETS + block_target).astype(jnp.int32)
        return running.at[dest_rows].add(-updates)

    return lax.fori_loop(0, N_COL, add_device, running)
```

```python
import functools

import jax
import jax.numpy as jnp
import numpy as np
from jax import lax
from jax.experimental import pallas as pl
from jax.experimental.pallas import tpu as pltpu
from jax.sharding import PartitionSpec as P

MESH = pl.DeviceIdType.MESH


def place_slots(src_block, dest_owner, target, counts, peer_count, capacity):
    slot_count = src_block.shape[1]
    slot_index = jnp.arange(slot_count, dtype=jnp.int32)
    owner_rank = dest_owner[:, 0]
    matches = (owner_rank[:, None] == jnp.arange(peer_count, dtype=jnp.int32)[None, :]).astype(
        jnp.int32
    )
    earlier = jnp.cumsum(matches, axis=0) - matches
    rank_in = jnp.sum(earlier * matches, axis=1)
    position = owner_rank * capacity + rank_in
    is_live = slot_index < counts[0]
    routed = jnp.zeros((peer_count * capacity,), jnp.int32).at[position].set(target)
    return (src_block[0], position, is_live, routed.reshape(peer_count, capacity))


def pack_updates(flat_updates, chosen, position, is_live, peer_count, capacity):
    picked = flat_updates[chosen]
    picked = jnp.where(is_live[:, None, None], picked, jnp.zeros_like(picked))
    buffer = (
        jnp.zeros((peer_count * capacity,) + picked.shape[1:], picked.dtype)
        .at[position]
        .set(picked)
    )
    return buffer.reshape((peer_count, capacity) + picked.shape[1:])


def assemble(received, labels, targets):
    arrived = received.reshape((-1,) + received.shape[2:])
    flat_labels = labels.reshape(-1)
    select = (flat_labels[None, :] == jnp.arange(targets, dtype=jnp.int32)[:, None]).astype(
        jnp.bfloat16
    )
    return jnp.einsum("tn,nrc->trc", select, arrived, preferred_element_type=jnp.float32)


def pair_products(own_rows, piece_rows):
    blocks = own_rows.shape[1]
    upper_table = np.array([a for a in range(blocks) for b in range(a + 1)], np.int32)
    lower_table = np.array([b for a in range(blocks) for b in range(a + 1)], np.int32)
    left_rows = own_rows[:, upper_table]
    right_rows = piece_rows[:, lower_table]
    return jnp.einsum(
        "fprw,fpcw->fprc", left_rows, right_rows, preferred_element_type=jnp.float32
    ).astype(jnp.bfloat16)


def plan(quarter):
    sizes = [quarter // 4] * 3 + [quarter // 8] * 2
    ends = [sum(sizes[: k + 1]) for k in range(len(sizes))]
    middle = ends.index(quarter // 2)
    units = [("own", 0, quarter)]
    for k, size in enumerate(sizes):
        if k == middle:
            units.append(("cross", k, quarter // 2))
        if k > middle:
            units.append(("tie", k, size))
        units.append(("near", k, 2 * size))
    return sizes, ends, middle, units


def kernel(
    chips, capacity, src_block, owner, target, counts, own, parent, out,
    table, from_x, from_y, product, kept, summed, to_pair, from_pair, to_chip, from_chip,
    to_back, from_back,
    x_send, x_recv, y_send, y_recv, p_send, p_recv, z_send, z_recv, b_send, b_recv,
):
    fronts, blocks, quarter, width = own.shape
    targets = parent.shape[0]
    pairs = blocks * (blocks + 1) // 2
    slots = src_block.shape[1]
    half = quarter // 2
    sizes, ends, middle, units = plan(quarter)
    last = len(sizes) - 1
    unit_of = {(kind, k): u for u, (kind, k, _) in enumerate(units)}
    g, c = lax.axis_index("grp"), lax.axis_index("col")
    gy, gx = g // 2, g % 2
    z, core = c // 2, c % 2
    x_peer = gy * 2 + (1 - gx)
    y_peer = (1 - gy) * 2 + gx
    d_peer = 3 - g
    to_x, to_y = {"grp": x_peer, "col": c}, {"grp": y_peer, "col": c}
    to_core = {"grp": g, "col": z * 2 + 1 - core}
    far = [lax.rem(z + hop, chips) for hop in range(1, chips)]
    to_far = [{"grp": g, "col": chip * 2 + core} for chip in far]

    barrier = pltpu.get_barrier_semaphore()
    peers = [to_x, to_y, to_core] + to_far
    for peer in peers:
        pl.semaphore_signal(barrier, inc=1, device_id=peer, device_id_type=MESH)
    pl.semaphore_wait(barrier, len(peers))

    def remote(src, dst, send, recv, device):
        return pltpu.make_async_remote_copy(
            src_ref=src, dst_ref=dst, send_sem=send, recv_sem=recv,
            device_id=device, device_id_type=MESH,
        )

    def x_rows(k):
        return slice(ends[k] - sizes[k], ends[k])

    def y_rows(k):
        return slice(quarter - ends[k], quarter - ends[k] + sizes[k])

    def static(rows):
        return pl.ds(rows.start, rows.stop - rows.start)

    x_copy, y_copy = [], []
    for k in range(len(sizes)):
        at_x, at_y = static(x_rows(k)), static(y_rows(k))
        x_copy.append(
            remote(own.at[:, :, at_x], from_x.at[:, :, at_x], x_send.at[k], x_recv.at[k], to_x)
        )
        y_copy.append(
            remote(own.at[:, :, at_y], from_y.at[:, :, at_y], y_send.at[k], y_recv.at[k], to_y)
        )
        x_copy[k].start()
        y_copy[k].start()

    bits = (fronts * pairs * 8 - 1).bit_length()
    per_word = 31 // bits
    words = -(-capacity // per_word)
    mask = (1 << (bits * per_word)) - 1

    def list_owners(first, count):
        def look(s, state):
            value = src_block[0, s] * 8 + jnp.where(s < counts[0], target[0, s] + 1, 0)
            named = owner[0, s]
            after = []
            for i in range(count):
                mine = named == first + i
                held = state[i * words:(i + 1) * words]
                carry = value
                for word in held:
                    moved = ((word << bits) & mask) | carry
                    carry = word >> (bits * (per_word - 1))
                    after.append(jnp.where(mine, moved, word))
            return tuple(after)

        state = lax.fori_loop(0, slots, look, (jnp.int32(0),) * (words * count))
        for i in range(count):
            for k in range(capacity):
                word = state[i * words + k // per_word]
                item = (word >> (bits * (k % per_word))) & ((1 << bits) - 1)
                table[0, (first + i) * capacity + k] = item >> 3
                table[1, (first + i) * capacity + k] = item & 7

    for first in range(0, 2 * chips, 4):
        list_owners(first, min(4, 2 * chips - first))

    p_copy, z_copy = [], []
    for u in range(len(units)):
        p_copy.append(remote(to_pair[u], from_pair[u], p_send.at[u], p_recv.at[u], to_core))
        z_copy.append([
            remote(
                to_chip[u].at[h], from_chip[u].at[h],
                z_send.at[u, h], z_recv.at[u, h], to_far[h],
            )
            for h in range(chips - 1)
        ])

    def select(high, parity, store):
        tile = min(32, high)

        def chip(zz, carry):
            base = (zz * 2 + parity) * capacity
            chosen = [table[0, base + k] for k in range(capacity)]
            label = [table[1, base + k] for k in range(capacity)]
            weight = [
                [jnp.where(label[k] == t + 1, 1.0, 0.0).astype(jnp.float32) for t in range(targets)]
                for k in range(capacity)
            ]

            def rows(i, carry):
                start = pl.multiple_of(i * tile, tile)
                taken = [
                    product[chosen[k], pl.ds(start, tile), :].astype(jnp.float32)
                    for k in range(capacity)
                ]
                for t in range(targets):
                    total = taken[0] * weight[0][t]
                    for k in range(1, capacity):
                        total = total + taken[k] * weight[k][t]
                    store(zz, t, start, tile, total)
                return carry

            return lax.fori_loop(0, high // tile, rows, carry)

        lax.fori_loop(0, chips, chip, 0)

    def dot(left, right):
        return lax.dot_general(
            left, right, (((1,), (1,)), ((), ())), preferred_element_type=jnp.float32
        ).astype(jnp.bfloat16)

    def stack(f, parts):
        return [jnp.concatenate([ref[f, b, rows] for ref, rows in parts], axis=0) for b in range(blocks)]

    every = slice(0, quarter)

    def against_own(f, parts, high):
        left = stack(f, parts)
        for first in range(0, blocks, 2):
            width_of = min(2, blocks - first)
            right = jnp.concatenate([own[f, first + i] for i in range(width_of)], axis=0)
            made = dot(jnp.concatenate(left[:first + width_of], axis=0), right)
            for i in range(width_of):
                a = first + i
                for b in range(a + 1):
                    product[f * pairs + a * (a + 1) // 2 + b, :high] = made[
                        b * high:(b + 1) * high, i * quarter:(i + 1) * quarter
                    ]

    def grid(f, left, left_rows, right, right_rows):
        return dot(
            jnp.concatenate(stack(f, [(left, left_rows)]), axis=0),
            jnp.concatenate(stack(f, [(right, right_rows)]), axis=0),
        )

    def paired(f, high, lower, upper):
        for a in range(blocks):
            for b in range(a + 1):
                product[f * pairs + a * (a + 1) // 2 + b, :high] = jnp.concatenate(
                    [lower(a, b), upper(a, b)], axis=1
                )

    def make(u):
        kind, k, high = units[u]

        def front(f, carry):
            if kind == "own":
                against_own(f, [(own, every)], high)
            elif kind == "near":
                against_own(f, [(from_x, x_rows(k)), (from_y, y_rows(k))], high)
            elif kind == "cross":
                made = grid(f, from_y, slice(half, quarter), from_x, slice(0, half))

                def piece(p, q):
                    return made[p * high:(p + 1) * high, q * half:(q + 1) * half]

                paired(f, high, lambda a, b: piece(b, a), lambda a, b: piece(a, b))
            else:
                by_y = grid(f, from_y, y_rows(k), from_x, slice(0, half))
                by_x = grid(f, from_x, x_rows(k), from_y, slice(half, quarter))

                def piece(made, p, q):
                    return made[p * high:(p + 1) * high, q * half:(q + 1) * half]

                paired(
                    f, high, lambda a, b: piece(by_y, b, a), lambda a, b: piece(by_x, a, b)
                )
            return carry

        lax.fori_loop(0, fronts, front, 0)

        def store_pair(zz, t, start, tile, total):
            to_pair[u][zz, t, pl.ds(start, tile), :] = total.astype(jnp.bfloat16)

        def store_kept(zz, t, start, tile, total):
            kept[u][zz, t, pl.ds(start, tile), :] = total

        select(high, 1 - core, store_pair)
        p_copy[u].start()
        select(high, core, store_kept)

    def pass_on(u):
        p_copy[u].wait_recv()
        for h in range(chips - 1):
            to_chip[u][h] = (
                kept[u][far[h]] + from_pair[u][far[h]].astype(jnp.float32)
            ).astype(jnp.bfloat16)
            z_copy[u][h].start()
        summed[u][...] = kept[u][z] + from_pair[u][z].astype(jnp.float32)

    def finish(u):
        for h in range(chips - 1):
            z_copy[u][h].wait_recv()
        total = summed[u][...]
        for h in range(chips - 1):
            total = total + from_chip[u][h].astype(jnp.float32)
        return total

    def settle(u):
        summed[u][...] = finish(u)

    corner = [unit_of["cross", middle]] + [unit_of["tie", k] for k in range(middle + 1, last + 1)]
    back = []

    def send_back(i):
        to_back[i][...] = finish(corner[i]).astype(jnp.bfloat16)
        back.append(remote(to_back[i], from_back[i], b_send.at[i], b_recv.at[i], to_x))
        back[-1].start()
        if i == 0:
            at = len(corner)
            back.append(remote(to_back[0], from_back[at], b_send.at[at], b_recv.at[at], to_y))
            back[-1].start()

    def write(member, total_of):
        at = pl.ds(pl.multiple_of(member * quarter, quarter), quarter)
        for t in range(targets):
            out[t, :, at] = parent[t, :, at] - total_of(t)

    def near_x(t):
        return jnp.concatenate(
            [summed[unit_of["near", k]][t, :sizes[k]] for k in range(len(sizes))], axis=0
        ).T

    def near_y(t):
        return jnp.concatenate(
            [summed[unit_of["near", k]][t, sizes[k]:] for k in reversed(range(len(sizes)))], axis=0
        ).T

    def diagonal(t):
        ties = list(range(1, len(corner)))
        turned = jnp.concatenate(
            [from_back[i][t].astype(jnp.float32) for i in reversed(ties)]
            + [from_back[0][t].astype(jnp.float32)],
            axis=0,
        )
        upper = turned.T[:half]
        tied = jnp.concatenate([from_back[i][t].astype(jnp.float32) for i in ties], axis=0)
        crossed = from_back[len(corner)][t].astype(jnp.float32)
        lower = jnp.concatenate([crossed[:, half:], tied[:, half:]], axis=1)
        return jnp.concatenate([upper, lower], axis=0)

    def arrive(k):
        x_copy[k].wait_recv()
        y_copy[k].wait_recv()

    u_own = unit_of["own", 0]
    make(u_own)
    pass_on(u_own)
    for k in range(len(sizes)):
        arrive(k)
        new = [unit_of[kind, k] for kind in ("cross", "tie", "near") if (kind, k) in unit_of]
        for u in new:
            make(u)
        for u in new:
            pass_on(u)
        if k == middle:
            settle(u_own)
            write(g, lambda t: summed[u_own][t].T)
        if k > 0:
            settle(unit_of["near", k - 1])
        if k > middle:
            send_back(k - 1 - middle)
    send_back(len(corner) - 1)
    settle(unit_of["near", last])
    write(x_peer, near_x)
    write(y_peer, near_y)
    for copy in back:
        copy.wait_recv()
    write(d_peer, diagonal)
    for copy in x_copy + y_copy + p_copy + back:
        copy.wait_send()
    for row in z_copy:
        for copy in row:
            copy.wait_send()


def fused(panels, parent, src_block, dest_owner, target, counts, chips, capacity):
    fronts, blocks, quarter, width = panels.shape
    targets = parent.shape[0]
    pairs = blocks * (blocks + 1) // 2
    sizes, _, middle, units = plan(quarter)
    heights = [high for _, _, high in units]
    corner = [high for kind, _, high in units if kind in ("cross", "tie")]

    def buffers(count, kind=jnp.bfloat16):
        return [pltpu.VMEM((count, targets, high, quarter), kind) for high in heights]

    def backs(highs):
        return [pltpu.VMEM((targets, high, quarter), jnp.bfloat16) for high in highs]

    whole = pltpu.VMEM((fronts, blocks, quarter, width), panels.dtype)
    dma = pltpu.SemaphoreType.DMA
    scalars = pl.BlockSpec(memory_space=pltpu.SMEM)
    arrays = pl.BlockSpec(memory_space=pltpu.VMEM)
    return pl.pallas_call(
        functools.partial(kernel, chips, capacity),
        out_shape=jax.ShapeDtypeStruct(parent.shape, parent.dtype),
        in_specs=[scalars] * 4 + [arrays] * 2,
        out_specs=arrays,
        scratch_shapes=[
            pltpu.SMEM((2, 2 * chips * capacity), jnp.int32),
            whole, whole,
            pltpu.VMEM((fronts * pairs, quarter, quarter), jnp.bfloat16),
            buffers(chips, jnp.float32),
            [pltpu.VMEM((targets, high, quarter), jnp.float32) for high in heights],
            buffers(chips), buffers(chips), buffers(chips - 1), buffers(chips - 1),
            backs(corner), backs(corner + corner[:1]),
            dma((len(sizes),)), dma((len(sizes),)), dma((len(sizes),)), dma((len(sizes),)),
            dma((len(units),)), dma((len(units),)),
            dma((len(units), chips - 1)), dma((len(units), chips - 1)),
            dma((len(corner) + 1,)), dma((len(corner) + 1,)),
        ],
        compiler_params=pltpu.CompilerParams(
            collective_id=0, has_side_effects=True, vmem_limit_bytes=60 * 1024 * 1024
        ),
    )(src_block, dest_owner.reshape(1, -1), target.reshape(1, -1), counts, panels, parent)


def per_device(panels, parent, src_block, dest_owner, target, counts):
    fronts, blocks, quarter, _ = panels.shape
    pair_count = blocks * (blocks + 1) // 2
    peer_count = lax.axis_size("col")
    slot_count = src_block.shape[1]
    capacity = (slot_count + peer_count - 1) // peer_count + slot_count // (2 * peer_count)
    targets = parent.shape[0]
    if lax.axis_size("grp") == 4 and peer_count % 2 == 0 and targets < capacity and quarter == 128:
        return fused(
            panels, parent, src_block, dest_owner, target, counts, peer_count // 2, capacity
        )
    chosen, position, is_live, routed = place_slots(
        src_block, dest_owner, target, counts, peer_count, capacity
    )
    products = pair_products(panels, lax.all_gather(panels, "grp", axis=2, tiled=True))
    flat_updates = products.reshape(fronts * pair_count, quarter, products.shape[3])
    buffer = pack_updates(flat_updates, chosen, position, is_live, peer_count, capacity)
    received, labels = (
        lax.all_to_all(buffer, "col", split_axis=0, concat_axis=0, tiled=True),
        lax.all_to_all(routed, "col", split_axis=0, concat_axis=0, tiled=True),
    )
    return parent - assemble(received, labels, targets)


def solution(mesh):
    placed = (
        P("col", None, "grp", None),
        P("col", "grp", None),
        P("col", None),
        P("col", None),
        P("col"),
        P("col"),
    )
    return jax.shard_map(
        per_device, mesh=mesh, in_specs=placed, out_specs=P("col", "grp", None), check_vma=False
    )
```

```python
import functools

import jax
import jax.numpy as jnp
import numpy as np
from jax import lax
from jax.experimental import pallas as pl
from jax.experimental.pallas import tpu as pltpu
from jax.sharding import PartitionSpec as P

MESH = pl.DeviceIdType.MESH


def place_slots(src_block, dest_owner, target, counts, peer_count, capacity):
    slot_count = src_block.shape[1]
    slot_index = jnp.arange(slot_count, dtype=jnp.int32)
    owner_rank = dest_owner[:, 0]
    matches = (owner_rank[:, None] == jnp.arange(peer_count, dtype=jnp.int32)[None, :]).astype(
        jnp.int32
    )
    earlier = jnp.cumsum(matches, axis=0) - matches
    rank_in = jnp.sum(earlier * matches, axis=1)
    position = owner_rank * capacity + rank_in
    is_live = slot_index < counts[0]
    routed = jnp.zeros((peer_count * capacity,), jnp.int32).at[position].set(target)
    return (src_block[0], position, is_live, routed.reshape(peer_count, capacity))


def pack_updates(flat_updates, chosen, position, is_live, peer_count, capacity):
    picked = flat_updates[chosen]
    picked = jnp.where(is_live[:, None, None], picked, jnp.zeros_like(picked))
    buffer = (
        jnp.zeros((peer_count * capacity,) + picked.shape[1:], picked.dtype)
        .at[position]
        .set(picked)
    )
    return buffer.reshape((peer_count, capacity) + picked.shape[1:])


def assemble(received, labels, targets):
    arrived = received.reshape((-1,) + received.shape[2:])
    flat_labels = labels.reshape(-1)
    select = (flat_labels[None, :] == jnp.arange(targets, dtype=jnp.int32)[:, None]).astype(
        jnp.bfloat16
    )
    return jnp.einsum("tn,nrc->trc", select, arrived, preferred_element_type=jnp.float32)


def pair_products(own_rows, piece_rows):
    blocks = own_rows.shape[1]
    upper_table = np.array([a for a in range(blocks) for b in range(a + 1)], np.int32)
    lower_table = np.array([b for a in range(blocks) for b in range(a + 1)], np.int32)
    left_rows = own_rows[:, upper_table]
    right_rows = piece_rows[:, lower_table]
    return jnp.einsum(
        "fprw,fpcw->fprc", left_rows, right_rows, preferred_element_type=jnp.float32
    ).astype(jnp.bfloat16)


def plan(quarter):
    sizes = [quarter // 4] + [quarter // 8] * 6
    ends = [sum(sizes[: k + 1]) for k in range(len(sizes))]
    middle = ends.index(quarter // 2)
    units = [("own", -1, quarter)]
    for k, size in enumerate(sizes):
        if k == middle:
            units.append(("cross", k, quarter // 2))
        if k > middle:
            units.append(("tie", k, size))
        units.append(("near", k, 2 * size))
    return sizes, ends, middle, units


def kernel(
    chips, capacity, relays, src_block, owner, target, counts, panels, parent_in, out,
    table, own, parent, from_x, from_y, product, kept, summed, to_pair, from_pair,
    to_chip, from_chip, cargo, to_back, from_back, to_home, from_home,
    x_send, x_recv, y_send, y_recv, p_send, p_recv, z_send, z_recv, c_recv, b_send, b_recv,
    h_send, h_recv, l_sem,
):
    fronts, blocks, quarter, width = own.shape
    load_own = pltpu.make_async_copy(panels, own, l_sem.at[0])
    load_parent = pltpu.make_async_copy(parent_in, parent, l_sem.at[1])
    load_own.start()
    load_parent.start()
    targets = parent.shape[0]
    pairs = blocks * (blocks + 1) // 2
    slots = src_block.shape[1]
    half = quarter // 2
    sizes, ends, middle, units = plan(quarter)
    last = len(sizes) - 1
    unit_of = {(kind, k): u for u, (kind, k, _) in enumerate(units)}
    g, c = lax.axis_index("grp"), lax.axis_index("col")
    gy, gx = g // 2, g % 2
    z, core = c // 2, c % 2
    x_peer = gy * 2 + (1 - gx)
    y_peer = (1 - gy) * 2 + gx
    d_peer = 3 - g
    to_x, to_y = {"grp": x_peer, "col": c}, {"grp": y_peer, "col": c}
    to_core = {"grp": g, "col": z * 2 + 1 - core}
    far = [lax.rem(z + hop, chips) for hop in range(1, chips)]
    to_far = [{"grp": g, "col": chip * 2 + core} for chip in far]
    edge = jnp.logical_or(z == 0, z == chips - 1)
    beside = z + 1 - 2 * (z % 2)
    inner = jnp.where(z < 2, 2, 1)
    outer = jnp.where(z < 2, 3, 0)
    to_beside, to_inner, to_outer = (
        {"grp": g, "col": chip * 2 + core} for chip in (beside, inner, outer)
    )
    homes = [z] + far
    to_homes = [{"grp": x_peer, "col": chip * 2 + core} for chip in homes]

    barrier = pltpu.get_barrier_semaphore()
    peers = [to_y, to_core] + to_far + to_homes
    for peer in peers:
        pl.semaphore_signal(barrier, inc=1, device_id=peer, device_id_type=MESH)
    pl.semaphore_wait(barrier, len(peers))

    def remote(src, dst, send, recv, device):
        return pltpu.make_async_remote_copy(
            src_ref=src, dst_ref=dst, send_sem=send, recv_sem=recv,
            device_id=device, device_id_type=MESH,
        )

    def x_rows(k):
        return slice(ends[k] - sizes[k], ends[k])

    def y_rows(k):
        return slice(quarter - ends[k], quarter - ends[k] + sizes[k])

    def static(rows):
        return pl.ds(rows.start, rows.stop - rows.start)

    load_own.wait()
    x_copy, y_copy = [], []
    for k in range(len(sizes)):
        at_x, at_y = static(x_rows(k)), static(y_rows(k))
        x_copy.append(
            remote(own.at[:, :, at_x], from_x.at[:, :, at_x], x_send.at[k], x_recv.at[k], to_x)
        )
        y_copy.append(
            remote(own.at[:, :, at_y], from_y.at[:, :, at_y], y_send.at[k], y_recv.at[k], to_y)
        )
        x_copy[k].start()
        y_copy[k].start()

    bits = (fronts * pairs * 8 - 1).bit_length()
    per_word = 31 // bits
    words = -(-capacity // per_word)
    mask = (1 << (bits * per_word)) - 1

    def list_owners(first, count):
        def look(s, state):
            value = src_block[0, s] * 8 + jnp.where(s < counts[0], target[0, s] + 1, 0)
            named = owner[0, s]
            after = []
            for i in range(count):
                mine = named == first + i
                held = state[i * words:(i + 1) * words]
                carry = value
                for word in held:
                    moved = ((word << bits) & mask) | carry
                    carry = word >> (bits * (per_word - 1))
                    after.append(jnp.where(mine, moved, word))
            return tuple(after)

        state = lax.fori_loop(0, slots, look, (jnp.int32(0),) * (words * count))
        for i in range(count):
            for k in range(capacity):
                word = state[i * words + k // per_word]
                item = (word >> (bits * (k % per_word))) & ((1 << bits) - 1)
                table[0, (first + i) * capacity + k] = item >> 3
                table[1, (first + i) * capacity + k] = item & 7

    for first in range(0, 2 * chips, 4):
        list_owners(first, min(4, 2 * chips - first))

    def blocks_out(u):
        if relays[u]:
            to, slots_at = [to_beside, to_inner, to_outer], [0, 1, 1]
        else:
            to, slots_at = to_far, [0, 1, 2]
        return [
            remote(
                to_chip[u].at[h], from_chip[u].at[slots_at[h]],
                z_send.at[u, h], z_recv.at[u, slots_at[h]], to[h],
            )
            for h in range(chips - 1)
        ]

    p_copy, z_copy, c_copy = [], [], []
    for u in range(len(units)):
        p_copy.append(remote(to_pair[u], from_pair[u], p_send.at[u], p_recv.at[u], to_core))
        z_copy.append(blocks_out(u))
        c_copy.append([
            remote(
                to_chip[u].at[h], cargo[u].at[h - 1],
                z_send.at[u, h], c_recv.at[u, h - 1], to_beside,
            )
            for h in range(1, chips - 1)
        ] if relays[u] else None)
    h_copy = [
        remote(to_home.at[h], from_home.at[h], h_send.at[h], h_recv.at[h], to_homes[h])
        for h in range(chips)
    ]

    def select(high, parity, store):
        tile = min(32, high)

        def chip(zz, carry):
            base = (zz * 2 + parity) * capacity
            chosen = [table[0, base + k] for k in range(capacity)]
            label = [table[1, base + k] for k in range(capacity)]
            weight = [
                [jnp.where(label[k] == t + 1, 1.0, 0.0).astype(jnp.float32) for t in range(targets)]
                for k in range(capacity)
            ]

            def rows(i, carry):
                start = pl.multiple_of(i * tile, tile)
                taken = [
                    product[chosen[k], pl.ds(start, tile), :].astype(jnp.float32)
                    for k in range(capacity)
                ]
                for t in range(targets):
                    total = taken[0] * weight[0][t]
                    for k in range(1, capacity):
                        total = total + taken[k] * weight[k][t]
                    store(zz, t, start, tile, total)
                return carry

            return lax.fori_loop(0, high // tile, rows, carry, unroll=True)

        lax.fori_loop(0, chips, chip, 0)

    def dot(left, right):
        return lax.dot_general(
            left, right, (((1,), (1,)), ((), ())), preferred_element_type=jnp.float32
        ).astype(jnp.bfloat16)

    def stack(f, parts):
        return [jnp.concatenate([ref[f, b, rows] for ref, rows in parts], axis=0) for b in range(blocks)]

    every = slice(0, quarter)

    def against_own(f, parts, high):
        left = stack(f, parts)
        for first in range(0, blocks, 2):
            width_of = min(2, blocks - first)
            right = jnp.concatenate([own[f, first + i] for i in range(width_of)], axis=0)
            made = dot(jnp.concatenate(left[:first + width_of], axis=0), right)
            for i in range(width_of):
                a = first + i
                for b in range(a + 1):
                    product[f * pairs + a * (a + 1) // 2 + b, :high] = made[
                        b * high:(b + 1) * high, i * quarter:(i + 1) * quarter
                    ]

    def grid(f, left, left_rows, right, right_rows):
        return dot(
            jnp.concatenate(stack(f, [(left, left_rows)]), axis=0),
            jnp.concatenate(stack(f, [(right, right_rows)]), axis=0),
        )

    def paired(f, high, lower, upper):
        for a in range(blocks):
            for b in range(a + 1):
                product[f * pairs + a * (a + 1) // 2 + b, :high] = jnp.concatenate(
                    [lower(a, b), upper(a, b)], axis=1
                )

    def make(u):
        kind, k, high = units[u]

        def front(f, carry):
            if kind == "own":
                against_own(f, [(own, every)], high)
            elif kind == "near":
                against_own(f, [(from_x, x_rows(k)), (from_y, y_rows(k))], high)
            elif kind == "cross":
                made = grid(f, from_y, slice(half, quarter), from_x, slice(0, half))

                def piece(p, q):
                    return made[p * high:(p + 1) * high, q * half:(q + 1) * half]

                paired(f, high, lambda a, b: piece(b, a), lambda a, b: piece(a, b))
            else:
                by_y = grid(f, from_y, y_rows(k), from_x, slice(0, half))
                by_x = grid(f, from_x, x_rows(k), from_y, slice(half, quarter))

                def piece(made, p, q):
                    return made[p * high:(p + 1) * high, q * half:(q + 1) * half]

                paired(
                    f, high, lambda a, b: piece(by_y, b, a), lambda a, b: piece(by_x, a, b)
                )
            return carry

        lax.fori_loop(0, fronts, front, 0, unroll=True)

        def store_pair(zz, t, start, tile, total):
            to_pair[u][zz, t, pl.ds(start, tile), :] = total.astype(jnp.bfloat16)

        def store_kept(zz, t, start, tile, total):
            kept[u][zz, t, pl.ds(start, tile), :] = total

        select(high, 1 - core, store_pair)
        p_copy[u].start()
        select(high, core, store_kept)

    def paired_sum(u, chip):
        return kept[u][chip] + from_pair[u][chip].astype(jnp.float32)

    def pass_on(u):
        p_copy[u].wait_recv()
        if u == u_home:
            for h in range(chips):
                to_home[h] = paired_sum(u, homes[h]).astype(jnp.bfloat16)
                h_copy[h].start()
            return
        if not relays[u]:
            for h in range(chips - 1):
                to_chip[u][h] = paired_sum(u, far[h]).astype(jnp.bfloat16)
                z_copy[u][h].start()
        else:
            @pl.when(edge)
            def _():
                for h, chip in ((2, outer), (1, inner)):
                    to_chip[u][h] = paired_sum(u, chip).astype(jnp.bfloat16)
                    c_copy[u][h - 1].start()

            to_chip[u][0] = paired_sum(u, beside).astype(jnp.bfloat16)
            z_copy[u][0].start()
        summed[u][...] = paired_sum(u, z)

    def relay(u):
        @pl.when(jnp.logical_not(edge))
        def _():
            for h, chip in ((2, outer), (1, inner)):
                c_copy[u][h - 1].wait_recv()
                to_chip[u][h] = (
                    paired_sum(u, chip) + cargo[u][h - 1].astype(jnp.float32)
                ).astype(jnp.bfloat16)
                z_copy[u][h].start()

    def finish(u):
        count = 2 if relays[u] else chips - 1
        for h in range(count):
            z_copy[u][h].wait_recv()
        total = summed[u][...]
        for h in range(count):
            total = total + from_chip[u][h].astype(jnp.float32)
        return total

    def settle(u):
        summed[u][...] = finish(u)

    u_own, u_home = unit_of["own", -1], unit_of["tie", last]
    corner = [unit_of["cross", middle]] + [unit_of["tie", k] for k in range(middle + 1, last)]
    back = []

    def send_back(i):
        to_back[i][...] = finish(corner[i]).astype(jnp.bfloat16)
        back.append(remote(to_back[i], from_back[i], b_send.at[i], b_recv.at[i], to_x))
        back[-1].start()
        if i == 0:
            at = len(corner)
            back.append(remote(to_back[0], from_back[at], b_send.at[at], b_recv.at[at], to_y))
            back[-1].start()

    def write(member, total_of):
        at = pl.ds(pl.multiple_of(member * quarter, quarter), quarter)
        for t in range(targets):
            out[t, :, at] = parent[t, :, at] - total_of(t)

    def near_x(t):
        return jnp.concatenate(
            [summed[unit_of["near", k]][t, :sizes[k]] for k in range(len(sizes))], axis=0
        ).T

    def near_y(t):
        return jnp.concatenate(
            [summed[unit_of["near", k]][t, sizes[k]:] for k in reversed(range(len(sizes)))], axis=0
        ).T

    def diagonal(t):
        ties = [from_back[i][t].astype(jnp.float32) for i in range(1, len(corner))]
        newest = from_home[0, t].astype(jnp.float32)
        for h in range(1, chips):
            newest = newest + from_home[h, t].astype(jnp.float32)
        ties.append(newest)
        turned = jnp.concatenate(ties[::-1] + [from_back[0][t].astype(jnp.float32)], axis=0)
        upper = turned.T[:half]
        tied = jnp.concatenate(ties, axis=0)
        crossed = from_back[len(corner)][t].astype(jnp.float32)
        lower = jnp.concatenate([crossed[:, half:], tied[:, half:]], axis=1)
        return jnp.concatenate([upper, lower], axis=0)

    def arrive(k):
        x_copy[k].wait_recv()
        y_copy[k].wait_recv()

    make(u_own)
    pass_on(u_own)
    relay(u_own)
    load_parent.wait()
    for k in range(len(sizes)):
        arrive(k)
        new = [unit_of[kind, k] for kind in ("tie", "near", "cross") if (kind, k) in unit_of]
        for u in new:
            make(u)
        for u in new:
            pass_on(u)
        if k == middle:
            settle(u_own)
            write(g, lambda t: summed[u_own][t].T)
            settle(unit_of["near", 0])
        for u in new:
            if relays[u]:
                relay(u)
    for i in range(len(corner)):
        send_back(i)
    for k in range(1, last + 1):
        settle(unit_of["near", k])
    write(x_peer, near_x)
    write(y_peer, near_y)
    for copy in back + h_copy:
        copy.wait_recv()
    write(d_peer, diagonal)
    for copy in x_copy + y_copy + p_copy + back + h_copy:
        copy.wait_send()
    for u in range(len(units)):
        if u != u_home:
            for copy in z_copy[u]:
                copy.wait_send()


def fused(panels, parent, src_block, dest_owner, target, counts, chips, capacity):
    fronts, blocks, quarter, width = panels.shape
    targets = parent.shape[0]
    pairs = blocks * (blocks + 1) // 2
    sizes, _, middle, units = plan(quarter)
    heights = [high for _, _, high in units]
    corner = [high for kind, _, high in units if kind in ("cross", "tie")][:-1]
    relays = [k <= middle + 0 for _, k, _ in units]

    def buffers(count, kind=jnp.bfloat16):
        return [pltpu.VMEM((count, targets, high, quarter), kind) for high in heights]

    def backs(highs):
        return [pltpu.VMEM((targets, high, quarter), jnp.bfloat16) for high in highs]

    whole = pltpu.VMEM((fronts, blocks, quarter, width), panels.dtype)
    dma = pltpu.SemaphoreType.DMA
    scalars = pl.BlockSpec(memory_space=pltpu.SMEM)
    arrays = pl.BlockSpec(memory_space=pltpu.VMEM)
    there = pl.BlockSpec(memory_space=pl.ANY)
    home = pltpu.VMEM((chips, targets, units[-2][2], quarter), jnp.bfloat16)
    return pl.pallas_call(
        functools.partial(kernel, chips, capacity, relays),
        out_shape=pltpu.VMEM(parent.shape, parent.dtype),
        in_specs=[scalars] * 4 + [there] * 2,
        out_specs=arrays,
        scratch_shapes=[
            pltpu.SMEM((2, 2 * chips * capacity), jnp.int32),
            whole, pltpu.VMEM(parent.shape, parent.dtype), whole, whole,
            pltpu.VMEM((fronts * pairs, quarter, quarter), jnp.bfloat16),
            buffers(chips, jnp.float32),
            [pltpu.VMEM((targets, high, quarter), jnp.float32) for high in heights],
            buffers(chips), buffers(chips), buffers(chips - 1), buffers(chips - 1),
            buffers(chips - 2), backs(corner), backs(corner + corner[:1]), home, home,
            dma((len(sizes),)), dma((len(sizes),)), dma((len(sizes),)), dma((len(sizes),)),
            dma((len(units),)), dma((len(units),)),
            dma((len(units), chips - 1)), dma((len(units), chips - 1)),
            dma((len(units), chips - 2)), dma((len(corner) + 1,)), dma((len(corner) + 1,)),
            dma((chips,)), dma((chips,)), dma((2,)),
        ],
        compiler_params=pltpu.CompilerParams(
            collective_id=0, has_side_effects=True, vmem_limit_bytes=60 * 1024 * 1024
        ),
    )(src_block, dest_owner.reshape(1, -1), target.reshape(1, -1), counts, panels, parent)


def per_device(panels, parent, src_block, dest_owner, target, counts):
    fronts, blocks, quarter, _ = panels.shape
    pair_count = blocks * (blocks + 1) // 2
    peer_count = lax.axis_size("col")
    slot_count = src_block.shape[1]
    capacity = (slot_count + peer_count - 1) // peer_count + slot_count // (2 * peer_count)
    targets = parent.shape[0]
    if lax.axis_size("grp") == 4 and peer_count == 8 and targets < capacity and quarter == 128:
        return fused(
            panels, parent, src_block, dest_owner, target, counts, peer_count // 2, capacity
        )
    chosen, position, is_live, routed = place_slots(
        src_block, dest_owner, target, counts, peer_count, capacity
    )
    products = pair_products(panels, lax.all_gather(panels, "grp", axis=2, tiled=True))
    flat_updates = products.reshape(fronts * pair_count, quarter, products.shape[3])
    buffer = pack_updates(flat_updates, chosen, position, is_live, peer_count, capacity)
    received, labels = (
        lax.all_to_all(buffer, "col", split_axis=0, concat_axis=0, tiled=True),
        lax.all_to_all(routed, "col", split_axis=0, concat_axis=0, tiled=True),
    )
    return parent - assemble(received, labels, targets)


def solution(mesh):
    placed = (
        P("col", None, "grp", None),
        P("col", "grp", None),
        P("col", None),
        P("col", None),
        P("col"),
        P("col"),
    )
    return jax.shard_map(
        per_device, mesh=mesh, in_specs=placed, out_specs=P("col", "grp", None), check_vma=False
    )
```

```python
import functools

import jax
import jax.numpy as jnp
import numpy as np
from jax import lax
from jax.experimental import pallas as pl
from jax.experimental.pallas import tpu as pltpu
from jax.sharding import PartitionSpec as P

MESH = pl.DeviceIdType.MESH


def place_slots(src_block, dest_owner, target, counts, peer_count, capacity):
    slot_count = src_block.shape[1]
    slot_index = jnp.arange(slot_count, dtype=jnp.int32)
    owner_rank = dest_owner[:, 0]
    matches = (owner_rank[:, None] == jnp.arange(peer_count, dtype=jnp.int32)[None, :]).astype(
        jnp.int32
    )
    earlier = jnp.cumsum(matches, axis=0) - matches
    rank_in = jnp.sum(earlier * matches, axis=1)
    position = owner_rank * capacity + rank_in
    is_live = slot_index < counts[0]
    routed = jnp.zeros((peer_count * capacity,), jnp.int32).at[position].set(target)
    return (src_block[0], position, is_live, routed.reshape(peer_count, capacity))


def pack_updates(flat_updates, chosen, position, is_live, peer_count, capacity):
    picked = flat_updates[chosen]
    picked = jnp.where(is_live[:, None, None], picked, jnp.zeros_like(picked))
    buffer = (
        jnp.zeros((peer_count * capacity,) + picked.shape[1:], picked.dtype)
        .at[position]
        .set(picked)
    )
    return buffer.reshape((peer_count, capacity) + picked.shape[1:])


def assemble(received, labels, targets):
    arrived = received.reshape((-1,) + received.shape[2:])
    flat_labels = labels.reshape(-1)
    select = (flat_labels[None, :] == jnp.arange(targets, dtype=jnp.int32)[:, None]).astype(
        jnp.bfloat16
    )
    return jnp.einsum("tn,nrc->trc", select, arrived, preferred_element_type=jnp.float32)


def pair_products(own_rows, piece_rows):
    blocks = own_rows.shape[1]
    upper_table = np.array([a for a in range(blocks) for b in range(a + 1)], np.int32)
    lower_table = np.array([b for a in range(blocks) for b in range(a + 1)], np.int32)
    left_rows = own_rows[:, upper_table]
    right_rows = piece_rows[:, lower_table]
    return jnp.einsum(
        "fprw,fpcw->fprc", left_rows, right_rows, preferred_element_type=jnp.float32
    ).astype(jnp.bfloat16)


def plan(quarter):
    sizes = [quarter // 4] + [quarter // 8] * 6
    ends = [sum(sizes[: k + 1]) for k in range(len(sizes))]
    middle = ends.index(quarter // 2)
    units = [("own", -1, quarter)]
    for k, size in enumerate(sizes):
        if k == middle:
            units.append(("cross", k, quarter // 2))
        if k > middle:
            units.append(("tie", k, size))
        units.append(("near", k, 2 * size))
    return sizes, ends, middle, units


def layout(units, middle):
    relayed, direct = [], []
    for u, (kind, k, _) in enumerate(units):
        (relayed if k <= middle else direct).append(u)
    home = direct[-2]
    direct = [u for u in direct if u != home]
    first = {}
    counts = []
    for group in (relayed, direct):
        row = 0
        for u in group:
            first[u] = row
            row += units[u][2]
        counts.append(row)
    return relayed, direct, home, first, counts


def kernel(
    chips, capacity, src_block, owner, target, counts, panels, parent_in, out,
    table, own, parent, from_x, from_y, product, tie_product, kept, summed, to_pair, from_pair,
    to_chip, from_relay, from_direct, cargo, to_back, from_back, from_back_y, to_home, from_home,
    x_send, x_recv, y_send, y_recv, p_send, p_recv, z_send, z_recv, c_recv, b_send, b_recv,
    ready, h_send, h_recv, l_sem,
):
    fronts, blocks, quarter, width = own.shape
    share = quarter // 4
    load_own = [
        pltpu.make_async_copy(
            panels.at[:, :, pl.ds(i * share, share)], own.at[:, :, pl.ds(i * share, share)],
            l_sem.at[1 + i],
        )
        for i in range(4)
    ]
    load_parent = pltpu.make_async_copy(parent_in, parent, l_sem.at[0])
    for i in (0, 3, 1, 2):
        load_own[i].start()
    targets = parent.shape[0]
    pairs = blocks * (blocks + 1) // 2
    slots = src_block.shape[1]
    half = quarter // 2
    sizes, ends, middle, units = plan(quarter)
    last = len(sizes) - 1
    relayed, direct, u_home, first_row, (relay_rows, direct_rows) = layout(units, middle)
    unit_of = {(kind, k): u for u, (kind, k, _) in enumerate(units)}
    g, c = lax.axis_index("grp"), lax.axis_index("col")
    gy, gx = g // 2, g % 2
    z, core = c // 2, c % 2
    x_peer = gy * 2 + (1 - gx)
    y_peer = (1 - gy) * 2 + gx
    d_peer = 3 - g
    to_x, to_y = {"grp": x_peer, "col": c}, {"grp": y_peer, "col": c}
    to_core = {"grp": g, "col": z * 2 + 1 - core}
    far = [lax.rem(z + hop, chips) for hop in range(1, chips)]
    to_far = [{"grp": g, "col": chip * 2 + core} for chip in far]
    edge = jnp.logical_or(z == 0, z == chips - 1)
    beside = z + 1 - 2 * (z % 2)
    inner = jnp.where(z < 2, 2, 1)
    outer = jnp.where(z < 2, 3, 0)
    to_beside, to_inner, to_outer = (
        {"grp": g, "col": chip * 2 + core} for chip in (beside, inner, outer)
    )
    homes = far + [z]
    to_homes = [{"grp": x_peer, "col": chip * 2 + core} for chip in homes]

    barrier = pltpu.get_barrier_semaphore()

    def greet(semaphore, peers):
        for peer in peers:
            pl.semaphore_signal(semaphore, inc=1, device_id=peer, device_id_type=MESH)

    plane = [{"grp": peer, "col": z * 2} for peer in (x_peer, y_peer)]
    greet(barrier, plane)

    @pl.when(core == 1)
    def _():
        greet(barrier, [to_core])

    @pl.when(core == 0)
    def _():
        pl.semaphore_wait(barrier, 5)
        greet(ready.at[0], [to_core])

    @pl.when(core == 1)
    def _():
        pl.semaphore_wait(ready.at[0], 1)
        greet(barrier, to_far + to_homes[:-1])

    def meet_line():
        @pl.when(core == 1)
        def _():
            pl.semaphore_wait(barrier, 2 * (chips - 1))
            greet(ready.at[1], [to_core])

        @pl.when(core == 0)
        def _():
            pl.semaphore_wait(ready.at[1], 1)

    def remote(src, dst, send, recv, device):
        return pltpu.make_async_remote_copy(
            src_ref=src, dst_ref=dst, send_sem=send, recv_sem=recv,
            device_id=device, device_id_type=MESH,
        )

    def x_rows(k):
        return slice(ends[k] - sizes[k], ends[k])

    def y_rows(k):
        return slice(quarter - ends[k], quarter - ends[k] + sizes[k])

    def static(rows):
        return pl.ds(rows.start, rows.stop - rows.start)

    def panel_copies(rows_of, into, send, recv, to):
        copies = []
        for k in range(len(sizes)):
            rows = static(rows_of(k))
            parts = [slice(0, fronts)] if k < last else [slice(0, fronts // 2), slice(fronts // 2, fronts)]
            for part in parts:
                at = (static(part), slice(None), rows)
                copies.append(
                    remote(own.at[at], into.at[at], send.at[0], recv.at[len(copies)], to)
                )
        return copies

    x_copy = panel_copies(x_rows, from_x, x_send, x_recv, to_x)
    y_copy = panel_copies(y_rows, from_y, y_send, y_recv, to_y)
    load_own[0].wait()
    x_copy[0].start()
    load_own[3].wait()
    y_copy[0].start()
    load_own[1].wait()
    load_own[2].wait()
    load_parent.start()
    for i in range(1, len(x_copy)):
        x_copy[i].start()
        y_copy[i].start()

    bits = (fronts * pairs * 8 - 1).bit_length()
    per_word = 31 // bits
    words = -(-capacity // per_word)
    mask = (1 << (bits * per_word)) - 1

    def list_owners(first, count):
        def look(s, state):
            value = src_block[0, s] * 8 + jnp.where(s < counts[0], target[0, s] + 1, 0)
            named = owner[0, s]
            after = []
            for i in range(count):
                mine = named == first + i
                held = state[i * words:(i + 1) * words]
                carry = value
                for word in held:
                    moved = ((word << bits) & mask) | carry
                    carry = word >> (bits * (per_word - 1))
                    after.append(jnp.where(mine, moved, word))
            return tuple(after)

        state = lax.fori_loop(0, slots, look, (jnp.int32(0),) * (words * count))
        for i in range(count):
            for k in range(capacity):
                word = state[i * words + k // per_word]
                item = (word >> (bits * (k % per_word))) & ((1 << bits) - 1)
                table[0, (first + i) * capacity + k] = item >> 3
                table[1, (first + i) * capacity + k] = item & 7

    for first in range(0, 2 * chips, 4):
        list_owners(first, min(4, 2 * chips - first))

    def rows_in(u):
        return pl.ds(first_row[u], units[u][2])

    def rows_all(u):
        if u == u_home:
            return pl.ds(relay_rows + direct_rows, units[u][2])
        return pl.ds(first_row[u] + (0 if u in relayed else relay_rows), units[u][2])

    early = relayed[:2]
    z_group = {u: early.index(u) if u in early else 2 for u in relayed}
    z_group.update({u: 3 if u != direct[-1] else 4 for u in direct})

    def blocks_out(u):
        if u in relayed:
            to, slots_at, into = [to_beside, to_inner, to_outer], [0, 1, 1], from_relay
        else:
            to, slots_at, into = to_far, [0, 1, 2], from_direct
        return [
            remote(
                to_chip.at[h, :, rows_all(u)], into.at[slots_at[h], :, rows_in(u)],
                z_send.at[0], z_recv.at[z_group[u]], to[h],
            )
            for h in range(chips - 1)
        ]

    p_copy, z_copy, c_copy = {}, {}, {}
    for u in range(len(units)):
        p_copy[u] = remote(to_pair[u], from_pair[u], p_send.at[u], p_recv.at[u], to_core)
        if u != u_home:
            z_copy[u] = blocks_out(u)
    for i, u in enumerate(relayed):
        c_copy[u] = [
            remote(
                to_chip.at[h, :, rows_all(u)], cargo.at[h - 1, :, rows_in(u)],
                z_send.at[0], c_recv.at[i, h - 1], to_beside,
            )
            for h in range(1, chips - 1)
        ]
    h_copy = [
        remote(to_home.at[h], from_home.at[h], h_send.at[0], h_recv.at[0], to_homes[h])
        for h in range(chips)
    ]

    def select(made, high, parity, store):
        tile = min(32, high)

        def chip(zz, carry):
            base = (zz * 2 + parity) * capacity
            chosen = [table[0, base + k] for k in range(capacity)]
            label = [table[1, base + k] for k in range(capacity)]
            weight = [
                [jnp.where(label[k] == t + 1, 1.0, 0.0).astype(jnp.float32) for t in range(targets)]
                for k in range(capacity)
            ]

            def rows(i, carry):
                start = pl.multiple_of(i * tile, tile)
                taken = [
                    made[chosen[k], pl.ds(start, tile), :].astype(jnp.float32)
                    for k in range(capacity)
                ]
                for t in range(targets):
                    total = taken[0] * weight[0][t]
                    for k in range(1, capacity):
                        total = total + taken[k] * weight[k][t]
                    store(zz, t, start, tile, total)
                return carry

            return lax.fori_loop(0, high // tile, rows, carry, unroll=True)

        lax.fori_loop(0, chips, chip, 0, unroll=True)

    def dot(left, right):
        return lax.dot_general(
            left, right, (((1,), (1,)), ((), ())), preferred_element_type=jnp.float32
        ).astype(jnp.bfloat16)

    def stack(f, parts):
        return [jnp.concatenate([ref[f, b, rows] for ref, rows in parts], axis=0) for b in range(blocks)]

    every = slice(0, quarter)

    def against_own(f, parts, high):
        left = stack(f, parts)
        for first in range(0, blocks, 2):
            width_of = min(2, blocks - first)
            right = jnp.concatenate([own[f, first + i] for i in range(width_of)], axis=0)
            made = dot(jnp.concatenate(left[:first + width_of], axis=0), right)
            for i in range(width_of):
                a = first + i
                for b in range(a + 1):
                    product[f * pairs + a * (a + 1) // 2 + b, :high] = made[
                        b * high:(b + 1) * high, i * quarter:(i + 1) * quarter
                    ]

    def grid(f, left, left_rows, right, right_rows):
        return dot(
            jnp.concatenate(stack(f, [(left, left_rows)]), axis=0),
            jnp.concatenate(stack(f, [(right, right_rows)]), axis=0),
        )

    def paired(into, f, high, lower, upper):
        for a in range(blocks):
            for b in range(a + 1):
                into[f * pairs + a * (a + 1) // 2 + b, :high] = jnp.concatenate(
                    [lower(a, b), upper(a, b)], axis=1
                )

    def product_of(u):
        return tie_product if units[u][0] == "tie" else product

    def multiply(u, some):
        kind, k, high = units[u]

        def front(f, carry):
            if kind == "own":
                against_own(f, [(own, every)], high)
            elif kind == "near":
                against_own(f, [(from_x, x_rows(k)), (from_y, y_rows(k))], high)
            elif kind == "cross":
                made = grid(f, from_y, slice(half, quarter), from_x, slice(0, half))

                def piece(p, q):
                    return made[p * high:(p + 1) * high, q * half:(q + 1) * half]

                paired(product, f, high, lambda a, b: piece(b, a), lambda a, b: piece(a, b))
            else:
                by_y = grid(f, from_y, y_rows(k), from_x, slice(0, half))
                by_x = grid(f, from_x, x_rows(k), from_y, slice(half, quarter))

                def piece(made, p, q):
                    return made[p * high:(p + 1) * high, q * half:(q + 1) * half]

                paired(
                    tie_product, f, high, lambda a, b: piece(by_y, b, a), lambda a, b: piece(by_x, a, b)
                )
            return carry

        if some == slice(0, fronts):
            lax.fori_loop(0, fronts, front, 0, unroll=True)
        else:
            for f in range(some.start, some.stop):
                front(f, 0)

    def add_up(u):
        high = units[u][2]

        def store_pair(zz, t, start, tile, total):
            to_pair[u][zz, t, pl.ds(start, tile), :] = total.astype(jnp.bfloat16)

        def store_kept(zz, t, start, tile, total):
            kept[u][zz, t, pl.ds(start, tile), :] = total

        select(product_of(u), high, 1 - core, store_pair)
        p_copy[u].start()
        select(product_of(u), high, core, store_kept)

    def make(u):
        multiply(u, slice(0, fronts))
        add_up(u)

    def paired_sum(u, chip):
        return kept[u][chip] + from_pair[u][chip].astype(jnp.float32)

    def pass_on(u):
        p_copy[u].wait_recv()
        if u == u_home:
            for h in range(chips):
                to_home[h] = paired_sum(u, homes[h]).astype(jnp.bfloat16)
                h_copy[h].start()
            return
        at = rows_all(u)
        if u not in relayed:
            for h in range(chips - 1):
                to_chip[h, :, at] = paired_sum(u, far[h]).astype(jnp.bfloat16)
                z_copy[u][h].start()
        else:
            @pl.when(edge)
            def _():
                for h, chip in ((2, outer), (1, inner)):
                    to_chip[h, :, at] = paired_sum(u, chip).astype(jnp.bfloat16)
                    c_copy[u][h - 1].start()

            to_chip[0, :, at] = paired_sum(u, beside).astype(jnp.bfloat16)
            z_copy[u][0].start()
        summed[u][...] = paired_sum(u, z)

    def relay(u):
        @pl.when(jnp.logical_not(edge))
        def _():
            for h, chip in ((2, outer), (1, inner)):
                c_copy[u][h - 1].wait_recv()
                to_chip[h, :, rows_all(u)] = (
                    paired_sum(u, chip) + cargo[h - 1, :, rows_in(u)].astype(jnp.float32)
                ).astype(jnp.bfloat16)
                z_copy[u][h].start()

    def arrived(group):
        members = [u for u in z_group if z_group[u] == group]
        into, count = (from_relay, chips - 2) if members[0] in relayed else (from_direct, chips - 1)
        rows = pl.ds(first_row[members[0]], sum(units[u][2] for u in members))
        remote(
            to_chip.at[:count, :, rows], into.at[:, :, rows],
            z_send.at[0], z_recv.at[group], to_beside,
        ).wait_recv()

    def finish(u):
        into, count = (from_relay, chips - 2) if u in relayed else (from_direct, chips - 1)
        total = summed[u][...]
        for h in range(count):
            total = total + into[h, :, rows_in(u)].astype(jnp.float32)
        return total

    def settle(u):
        summed[u][...] = finish(u)

    u_own = unit_of["own", -1]
    corner = [unit_of["cross", middle]] + [unit_of["tie", k] for k in range(middle + 1, last)]
    corner_row = [sum(units[v][2] for v in corner[:i]) for i in range(len(corner) + 1)]
    back = [
        remote(to_back, from_back, b_send.at[0], b_recv.at[0], to_x),
        remote(to_back.at[:, :half], from_back_y, b_send.at[1], b_recv.at[1], to_y),
    ]

    def send_back():
        for i, u in enumerate(corner):
            to_back[:, corner_row[i]:corner_row[i + 1]] = finish(u).astype(jnp.bfloat16)
        for copy in back:
            copy.start()

    def write(member, total_of):
        at = pl.ds(pl.multiple_of(member * quarter, quarter), quarter)
        for t in range(targets):
            out[t, :, at] = parent[t, :, at] - total_of(t)

    def near_x(t):
        return jnp.concatenate(
            [summed[unit_of["near", k]][t, :sizes[k]] for k in range(len(sizes))], axis=0
        ).T

    def near_y(t):
        return jnp.concatenate(
            [summed[unit_of["near", k]][t, sizes[k]:] for k in reversed(range(len(sizes)))], axis=0
        ).T

    def diagonal(t):
        ties = [from_back[t, half:].astype(jnp.float32)]
        newest = from_home[0, t].astype(jnp.float32)
        for h in range(1, chips):
            newest = newest + from_home[h, t].astype(jnp.float32)
        ties.append(newest)
        falling = [newest] + [
            from_back[t, corner_row[i]:corner_row[i + 1]].astype(jnp.float32)
            for i in reversed(range(len(corner)))
        ]
        turned = jnp.concatenate(falling, axis=0)
        upper = turned.T[:half]
        tied = jnp.concatenate(ties, axis=0)
        crossed = from_back_y[t].astype(jnp.float32)
        lower = jnp.concatenate([crossed[:, half:], tied[:, half:]], axis=1)
        return jnp.concatenate([upper, lower], axis=0)

    def arrive(k):
        x_copy[k].wait_recv()
        y_copy[k].wait_recv()

    make(u_own)
    meet_line()
    pass_on(u_own)
    relay(u_own)
    load_parent.wait()
    for k in range(len(sizes)):
        new = [unit_of[kind, k] for kind in ("tie", "near", "cross") if (kind, k) in unit_of]
        arrive(k)
        if k < last:
            for u in new:
                make(u)
        else:
            for u in new:
                multiply(u, slice(0, fronts // 2))
            arrive(k + 1)
            for u in new:
                multiply(u, slice(fronts // 2, fronts))
                add_up(u)
        for u in new:
            pass_on(u)
        if k == middle:
            for group, u in enumerate(early):
                arrived(group)
                settle(u)
            write(g, lambda t: summed[u_own][t].T)
        for u in new:
            if u in relayed:
                relay(u)
    arrived(2)
    arrived(3)
    send_back()
    for k in range(1, last):
        settle(unit_of["near", k])
    arrived(4)
    settle(unit_of["near", last])
    write(x_peer, near_x)
    write(y_peer, near_y)
    for copy in back:
        copy.wait_recv()
    whole_home = remote(to_home, from_home, h_send.at[0], h_recv.at[0], to_x)
    whole_home.wait_recv()
    write(d_peer, diagonal)
    for copy in back + [
        whole_home,
        remote(own, from_x, x_send.at[0], x_recv.at[0], to_x),
        remote(own, from_y, y_send.at[0], y_recv.at[0], to_y),
        *p_copy.values(),
        remote(to_chip, to_chip, z_send.at[0], z_recv.at[0], to_beside),
    ]:
        copy.wait_send()


def fused(panels, parent, src_block, dest_owner, target, counts, chips, capacity):
    fronts, blocks, quarter, width = panels.shape
    targets = parent.shape[0]
    pairs = blocks * (blocks + 1) // 2
    sizes, _, middle, units = plan(quarter)
    heights = [high for _, _, high in units]
    relayed, direct, _, _, (relay_rows, direct_rows) = layout(units, middle)
    tie = units[-2][2]
    corner_rows = sum(high for kind, _, high in units if kind in ("cross", "tie")) - tie

    def buffer(count, rows):
        return pltpu.VMEM((count, targets, rows, quarter), jnp.bfloat16)

    def sums(lead):
        return [pltpu.VMEM(lead + (targets, high, quarter), jnp.float32) for high in heights]

    def back(rows):
        return pltpu.VMEM((targets, rows, quarter), jnp.bfloat16)

    whole = pltpu.VMEM((fronts, blocks, quarter, width), panels.dtype)
    dma = pltpu.SemaphoreType.DMA
    scalars = pl.BlockSpec(memory_space=pltpu.SMEM)
    arrays = pl.BlockSpec(memory_space=pltpu.VMEM)
    there = pl.BlockSpec(memory_space=pl.ANY)
    home = buffer(chips, tie)
    return pl.pallas_call(
        functools.partial(kernel, chips, capacity),
        out_shape=pltpu.VMEM(parent.shape, parent.dtype),
        in_specs=[scalars] * 4 + [there] * 2,
        out_specs=arrays,
        scratch_shapes=[
            pltpu.SMEM((2, 2 * chips * capacity), jnp.int32),
            whole, pltpu.VMEM(parent.shape, parent.dtype), whole, whole,
            pltpu.VMEM((fronts * pairs, quarter, quarter), jnp.bfloat16),
            pltpu.VMEM((fronts * pairs, tie, quarter), jnp.bfloat16),
            sums((chips,)), sums(()),
            [buffer(chips, high) for high in heights], [buffer(chips, high) for high in heights],
            buffer(chips - 1, relay_rows + direct_rows), buffer(chips - 2, relay_rows),
            buffer(chips - 1, direct_rows), buffer(chips - 2, relay_rows),
            back(corner_rows), back(corner_rows), back(quarter // 2), home, home,
            dma((1,)), dma((len(sizes) + 1,)), dma((1,)), dma((len(sizes) + 1,)),
            dma((len(units),)), dma((len(units),)), dma((1,)), dma((5,)), dma((len(relayed), chips - 2)),
            dma((2,)), dma((2,)),
            pltpu.SemaphoreType.REGULAR((2,)), dma((1,)), dma((1,)), dma((5,)),
        ],
        compiler_params=pltpu.CompilerParams(
            collective_id=0, has_side_effects=True, vmem_limit_bytes=60 * 1024 * 1024
        ),
    )(src_block, dest_owner.reshape(1, -1), target.reshape(1, -1), counts, panels, parent)


def per_device(panels, parent, src_block, dest_owner, target, counts):
    fronts, blocks, quarter, _ = panels.shape
    pair_count = blocks * (blocks + 1) // 2
    peer_count = lax.axis_size("col")
    slot_count = src_block.shape[1]
    capacity = (slot_count + peer_count - 1) // peer_count + slot_count // (2 * peer_count)
    targets = parent.shape[0]
    if lax.axis_size("grp") == 4 and peer_count == 8 and targets < capacity and quarter == 128:
        return fused(
            panels, parent, src_block, dest_owner, target, counts, peer_count // 2, capacity
        )
    chosen, position, is_live, routed = place_slots(
        src_block, dest_owner, target, counts, peer_count, capacity
    )
    products = pair_products(panels, lax.all_gather(panels, "grp", axis=2, tiled=True))
    flat_updates = products.reshape(fronts * pair_count, quarter, products.shape[3])
    buffer = pack_updates(flat_updates, chosen, position, is_live, peer_count, capacity)
    received, labels = (
        lax.all_to_all(buffer, "col", split_axis=0, concat_axis=0, tiled=True),
        lax.all_to_all(routed, "col", split_axis=0, concat_axis=0, tiled=True),
    )
    return parent - assemble(received, labels, targets)


def solution(mesh):
    placed = (
        P("col", None, "grp", None),
        P("col", "grp", None),
        P("col", None),
        P("col", None),
        P("col"),
        P("col"),
    )
    return jax.shard_map(
        per_device, mesh=mesh, in_specs=placed, out_specs=P("col", "grp", None), check_vma=False
    )
```

```python
import functools

import jax
import jax.numpy as jnp
import numpy as np
from jax import lax
from jax.experimental import pallas as pl
from jax.experimental.pallas import tpu as pltpu
from jax.sharding import PartitionSpec as P

MESH = pl.DeviceIdType.MESH


def place_slots(src_block, dest_owner, target, counts, peer_count, capacity):
    slot_count = src_block.shape[1]
    slot_index = jnp.arange(slot_count, dtype=jnp.int32)
    owner_rank = dest_owner[:, 0]
    matches = (owner_rank[:, None] == jnp.arange(peer_count, dtype=jnp.int32)[None, :]).astype(
        jnp.int32
    )
    earlier = jnp.cumsum(matches, axis=0) - matches
    rank_in = jnp.sum(earlier * matches, axis=1)
    position = owner_rank * capacity + rank_in
    is_live = slot_index < counts[0]
    routed = jnp.zeros((peer_count * capacity,), jnp.int32).at[position].set(target)
    return (src_block[0], position, is_live, routed.reshape(peer_count, capacity))


def pack_updates(flat_updates, chosen, position, is_live, peer_count, capacity):
    picked = flat_updates[chosen]
    picked = jnp.where(is_live[:, None, None], picked, jnp.zeros_like(picked))
    buffer = (
        jnp.zeros((peer_count * capacity,) + picked.shape[1:], picked.dtype)
        .at[position]
        .set(picked)
    )
    return buffer.reshape((peer_count, capacity) + picked.shape[1:])


def assemble(received, labels, targets):
    arrived = received.reshape((-1,) + received.shape[2:])
    flat_labels = labels.reshape(-1)
    select = (flat_labels[None, :] == jnp.arange(targets, dtype=jnp.int32)[:, None]).astype(
        jnp.bfloat16
    )
    return jnp.einsum("tn,nrc->trc", select, arrived, preferred_element_type=jnp.float32)


def pair_products(own_rows, piece_rows):
    blocks = own_rows.shape[1]
    upper_table = np.array([a for a in range(blocks) for b in range(a + 1)], np.int32)
    lower_table = np.array([b for a in range(blocks) for b in range(a + 1)], np.int32)
    left_rows = own_rows[:, upper_table]
    right_rows = piece_rows[:, lower_table]
    return jnp.einsum(
        "fprw,fpcw->fprc", left_rows, right_rows, preferred_element_type=jnp.float32
    ).astype(jnp.bfloat16)


def plan(quarter):
    sizes = [quarter // 4] + [quarter // 8] * 6
    ends = [sum(sizes[: k + 1]) for k in range(len(sizes))]
    middle = ends.index(quarter // 2)
    units = [("own", -1, quarter)]
    for k, size in enumerate(sizes):
        if k == middle:
            units.append(("cross", k, quarter // 2))
        if k > middle:
            units.append(("tie", k, size))
        units.append(("near", k, 2 * size))
    return sizes, ends, middle, units


def layout(units, middle):
    relayed, direct = [], []
    for u, (kind, k, _) in enumerate(units):
        (relayed if k <= middle else direct).append(u)
    home = direct[-2]
    direct = [u for u in direct if u != home]
    first = {}
    counts = []
    for group in (relayed, direct):
        row = 0
        for u in group:
            first[u] = row
            row += units[u][2]
        counts.append(row)
    return relayed, direct, home, first, counts


def kernel(
    chips, capacity, src_block_in, owner_in, target_in, counts_in, panels, parent_in, out,
    src_block, owner, target, counts, table, own, parent, from_x, from_y, product, tie_product, kept, summed, to_pair, from_pair,
    to_chip, from_relay, from_direct, cargo, to_back, from_back, from_back_y, to_home, from_home,
    x_send, x_recv, y_send, y_recv, p_send, p_recv, z_send, z_recv, c_recv, b_send, b_recv,
    ready, h_send, h_recv, l_sem,
):
    fronts, blocks, quarter, width = own.shape
    share = quarter // 4
    load_own = [
        pltpu.make_async_copy(
            panels.at[:, :, pl.ds(i * share, share)], own.at[:, :, pl.ds(i * share, share)],
            l_sem.at[1 + i],
        )
        for i in range(4)
    ]
    load_parent = pltpu.make_async_copy(parent_in, parent, l_sem.at[0])
    for i in (0, 3, 1, 2):
        load_own[i].start()
    load_slots = [
        pltpu.make_async_copy(given, kept_at, l_sem.at[5 + i])
        for i, (given, kept_at) in enumerate((
            (src_block_in, src_block), (owner_in, owner), (target_in, target), (counts_in, counts)
        ))
    ]
    for copy in load_slots:
        copy.start()
    targets = parent.shape[0]
    pairs = blocks * (blocks + 1) // 2
    slots = src_block.shape[1]
    half = quarter // 2
    sizes, ends, middle, units = plan(quarter)
    last = len(sizes) - 1
    relayed, direct, u_home, first_row, (relay_rows, direct_rows) = layout(units, middle)
    unit_of = {(kind, k): u for u, (kind, k, _) in enumerate(units)}
    g, c = lax.axis_index("grp"), lax.axis_index("col")
    gy, gx = g // 2, g % 2
    z, core = c // 2, c % 2
    x_peer = gy * 2 + (1 - gx)
    y_peer = (1 - gy) * 2 + gx
    d_peer = 3 - g
    to_x, to_y = {"grp": x_peer, "col": c}, {"grp": y_peer, "col": c}
    to_core = {"grp": g, "col": z * 2 + 1 - core}
    far = [lax.rem(z + hop, chips) for hop in range(1, chips)]
    to_far = [{"grp": g, "col": chip * 2 + core} for chip in far]
    edge = jnp.logical_or(z == 0, z == chips - 1)
    beside = z + 1 - 2 * (z % 2)
    inner = jnp.where(z < 2, 2, 1)
    outer = jnp.where(z < 2, 3, 0)
    to_beside, to_inner, to_outer = (
        {"grp": g, "col": chip * 2 + core} for chip in (beside, inner, outer)
    )
    homes = far + [z]
    to_homes = [{"grp": x_peer, "col": chip * 2 + core} for chip in homes]

    barrier = pltpu.get_barrier_semaphore()

    def greet(semaphore, peers):
        for peer in peers:
            pl.semaphore_signal(semaphore, inc=1, device_id=peer, device_id_type=MESH)

    plane = [{"grp": peer, "col": z * 2} for peer in (x_peer, y_peer)]
    greet(barrier, plane)

    @pl.when(core == 1)
    def _():
        greet(barrier, [to_core])

    @pl.when(core == 0)
    def _():
        pl.semaphore_wait(barrier, 5)
        greet(ready.at[0], [to_core])

    @pl.when(core == 1)
    def _():
        pl.semaphore_wait(ready.at[0], 1)

    def meet_line():
        @pl.when(core == 1)
        def _():
            pl.semaphore_wait(barrier, 2 * (chips - 1))
            greet(ready.at[1], [to_core])

        @pl.when(core == 0)
        def _():
            pl.semaphore_wait(ready.at[1], 1)

    def remote(src, dst, send, recv, device):
        return pltpu.make_async_remote_copy(
            src_ref=src, dst_ref=dst, send_sem=send, recv_sem=recv,
            device_id=device, device_id_type=MESH,
        )

    def x_rows(k):
        return slice(ends[k] - sizes[k], ends[k])

    def y_rows(k):
        return slice(quarter - ends[k], quarter - ends[k] + sizes[k])

    def static(rows):
        return pl.ds(rows.start, rows.stop - rows.start)

    def panel_copies(rows_of, into, send, recv, to):
        copies = []
        for k in range(len(sizes)):
            rows = static(rows_of(k))
            parts = [slice(0, fronts)] if k < last else [slice(f, f + 1) for f in range(fronts)]
            for part in parts:
                at = (static(part), slice(None), rows)
                copies.append(
                    remote(own.at[at], into.at[at], send.at[0], recv.at[len(copies)], to)
                )
        return copies

    x_copy = panel_copies(x_rows, from_x, x_send, x_recv, to_x)
    y_copy = panel_copies(y_rows, from_y, y_send, y_recv, to_y)
    load_own[0].wait()
    x_copy[0].start()
    load_own[3].wait()
    y_copy[0].start()
    load_own[1].wait()
    load_own[2].wait()
    load_parent.start()
    for i in range(1, len(x_copy)):
        x_copy[i].start()
        y_copy[i].start()

    @pl.when(core == 1)
    def _():
        greet(barrier, to_far + to_homes[:-1])

    bits = (fronts * pairs * 8 - 1).bit_length()
    per_word = 31 // bits
    words = -(-capacity // per_word)
    mask = (1 << (bits * per_word)) - 1

    def list_owners(first, count):
        def look(s, state):
            value = src_block[0, s] * 8 + jnp.where(s < counts[0, 0], target[0, s] + 1, 0)
            named = owner[0, s]
            after = []
            for i in range(count):
                mine = named == first + i
                held = state[i * words:(i + 1) * words]
                carry = value
                for word in held:
                    moved = ((word << bits) & mask) | carry
                    carry = word >> (bits * (per_word - 1))
                    after.append(jnp.where(mine, moved, word))
            return tuple(after)

        state = lax.fori_loop(0, slots, look, (jnp.int32(0),) * (words * count))
        for i in range(count):
            for k in range(capacity):
                word = state[i * words + k // per_word]
                item = (word >> (bits * (k % per_word))) & ((1 << bits) - 1)
                table[0, (first + i) * capacity + k] = item >> 3
                table[1, (first + i) * capacity + k] = item & 7

    for copy in load_slots:
        copy.wait()
    for first in range(0, 2 * chips, 4):
        list_owners(first, min(4, 2 * chips - first))

    def rows_in(u):
        return pl.ds(first_row[u], units[u][2])

    def rows_all(u):
        if u == u_home:
            return pl.ds(relay_rows + direct_rows, units[u][2])
        return pl.ds(first_row[u] + (0 if u in relayed else relay_rows), units[u][2])

    early = relayed[:2]
    z_group = {u: early.index(u) if u in early else 2 for u in relayed}
    z_group.update({u: 3 + max(0, units[u][1] - last + 2) for u in direct})

    def blocks_out(u):
        if u in relayed:
            to, slots_at, into = [to_beside, to_inner, to_outer], [0, 1, 1], from_relay
        else:
            to, slots_at, into = to_far, [0, 1, 2], from_direct
        return [
            remote(
                to_chip.at[h, :, rows_all(u)], into.at[slots_at[h], :, rows_in(u)],
                z_send.at[0], z_recv.at[z_group[u]], to[h],
            )
            for h in range(chips - 1)
        ]

    p_copy, z_copy, c_copy = {}, {}, {}
    for u in range(len(units)):
        p_copy[u] = remote(to_pair[u], from_pair[u], p_send.at[u], p_recv.at[u], to_core)
        if u != u_home:
            z_copy[u] = blocks_out(u)
    for i, u in enumerate(relayed):
        c_copy[u] = [
            remote(
                to_chip.at[h, :, rows_all(u)], cargo.at[h - 1, :, rows_in(u)],
                z_send.at[0], c_recv.at[i, h - 1], to_beside,
            )
            for h in range(1, chips - 1)
        ]
    h_copy = [
        remote(to_home.at[h], from_home.at[h], h_send.at[0], h_recv.at[0], to_homes[h])
        for h in range(chips)
    ]

    def select(made, high, parity, store):
        tile = min(32, high)

        def chip(zz, carry):
            base = (zz * 2 + parity) * capacity
            chosen = [table[0, base + k] for k in range(capacity)]
            label = [table[1, base + k] for k in range(capacity)]
            weight = [
                [jnp.where(label[k] == t + 1, 1.0, 0.0).astype(jnp.float32) for t in range(targets)]
                for k in range(capacity)
            ]

            def rows(i, carry):
                start = pl.multiple_of(i * tile, tile)
                taken = [
                    made[chosen[k], pl.ds(start, tile), :].astype(jnp.float32)
                    for k in range(capacity)
                ]
                for t in range(targets):
                    total = taken[0] * weight[0][t]
                    for k in range(1, capacity):
                        total = total + taken[k] * weight[k][t]
                    store(zz, t, start, tile, total)
                return carry

            return lax.fori_loop(0, high // tile, rows, carry, unroll=True)

        lax.fori_loop(0, chips, chip, 0, unroll=True)

    def dot(left, right):
        return lax.dot_general(
            left, right, (((1,), (1,)), ((), ())), preferred_element_type=jnp.float32
        ).astype(jnp.bfloat16)

    def stack(f, parts):
        return [jnp.concatenate([ref[f, b, rows] for ref, rows in parts], axis=0) for b in range(blocks)]

    every = slice(0, quarter)

    def against_own(f, parts, high):
        left = stack(f, parts)
        for first in range(0, blocks, 2):
            width_of = min(2, blocks - first)
            right = jnp.concatenate([own[f, first + i] for i in range(width_of)], axis=0)
            made = dot(jnp.concatenate(left[:first + width_of], axis=0), right)
            for i in range(width_of):
                a = first + i
                for b in range(a + 1):
                    product[f * pairs + a * (a + 1) // 2 + b, :high] = made[
                        b * high:(b + 1) * high, i * quarter:(i + 1) * quarter
                    ]

    def grid(f, left, left_rows, right, right_rows):
        return dot(
            jnp.concatenate(stack(f, [(left, left_rows)]), axis=0),
            jnp.concatenate(stack(f, [(right, right_rows)]), axis=0),
        )

    def paired(into, f, high, lower, upper):
        for a in range(blocks):
            for b in range(a + 1):
                into[f * pairs + a * (a + 1) // 2 + b, :high] = jnp.concatenate(
                    [lower(a, b), upper(a, b)], axis=1
                )

    def product_of(u):
        return tie_product if units[u][0] == "tie" else product

    def multiply(u, some):
        kind, k, high = units[u]

        def front(f, carry):
            if kind == "own":
                against_own(f, [(own, every)], high)
            elif kind == "near":
                against_own(f, [(from_x, x_rows(k)), (from_y, y_rows(k))], high)
            elif kind == "cross":
                made = grid(f, from_y, slice(half, quarter), from_x, slice(0, half))

                def piece(p, q):
                    return made[p * high:(p + 1) * high, q * half:(q + 1) * half]

                paired(product, f, high, lambda a, b: piece(b, a), lambda a, b: piece(a, b))
            else:
                by_y = grid(f, from_y, y_rows(k), from_x, slice(0, half))
                by_x = grid(f, from_x, x_rows(k), from_y, slice(half, quarter))

                def piece(made, p, q):
                    return made[p * high:(p + 1) * high, q * half:(q + 1) * half]

                paired(
                    tie_product, f, high, lambda a, b: piece(by_y, b, a), lambda a, b: piece(by_x, a, b)
                )
            return carry

        if some == slice(0, fronts):
            lax.fori_loop(0, fronts, front, 0, unroll=True)
        else:
            for f in range(some.start, some.stop):
                front(f, 0)

    def add_up(u):
        high = units[u][2]

        def store_pair(zz, t, start, tile, total):
            to_pair[u][zz, t, pl.ds(start, tile), :] = total.astype(jnp.bfloat16)

        def store_kept(zz, t, start, tile, total):
            kept[u][zz, t, pl.ds(start, tile), :] = total

        select(product_of(u), high, 1 - core, store_pair)
        p_copy[u].start()
        select(product_of(u), high, core, store_kept)

    def make(u):
        multiply(u, slice(0, fronts))
        add_up(u)

    def paired_sum(u, chip):
        return kept[u][chip] + from_pair[u][chip].astype(jnp.float32)

    def pass_on(u):
        p_copy[u].wait_recv()
        if u == u_home:
            for h in range(chips):
                to_home[h] = paired_sum(u, homes[h]).astype(jnp.bfloat16)
                h_copy[h].start()
            return
        at = rows_all(u)
        if u not in relayed:
            for h in range(chips - 1):
                to_chip[h, :, at] = paired_sum(u, far[h]).astype(jnp.bfloat16)
                z_copy[u][h].start()
        else:
            @pl.when(edge)
            def _():
                for h, chip in ((2, outer), (1, inner)):
                    to_chip[h, :, at] = paired_sum(u, chip).astype(jnp.bfloat16)
                    c_copy[u][h - 1].start()

            to_chip[0, :, at] = paired_sum(u, beside).astype(jnp.bfloat16)
            z_copy[u][0].start()
        summed[u][...] = paired_sum(u, z)

    def relay(u):
        @pl.when(jnp.logical_not(edge))
        def _():
            for h, chip in ((2, outer), (1, inner)):
                c_copy[u][h - 1].wait_recv()
                to_chip[h, :, rows_all(u)] = (
                    paired_sum(u, chip) + cargo[h - 1, :, rows_in(u)].astype(jnp.float32)
                ).astype(jnp.bfloat16)
                z_copy[u][h].start()

    def arrived(group):
        members = [u for u in z_group if z_group[u] == group]
        into, count = (from_relay, chips - 2) if members[0] in relayed else (from_direct, chips - 1)
        rows = pl.ds(first_row[members[0]], sum(units[u][2] for u in members))
        remote(
            to_chip.at[:count, :, rows], into.at[:, :, rows],
            z_send.at[0], z_recv.at[group], to_beside,
        ).wait_recv()

    def finish(u):
        into, count = (from_relay, chips - 2) if u in relayed else (from_direct, chips - 1)
        total = summed[u][...]
        for h in range(count):
            total = total + into[h, :, rows_in(u)].astype(jnp.float32)
        return total

    def settle(u):
        summed[u][...] = finish(u)

    u_own = unit_of["own", -1]
    corner = [unit_of["cross", middle]] + [unit_of["tie", k] for k in range(middle + 1, last)]
    corner_row = [sum(units[v][2] for v in corner[:i]) for i in range(len(corner) + 1)]
    split = corner_row[-2]
    back = [
        remote(to_back.at[:, :half], from_back_y, b_send.at[0], b_recv.at[0], to_y),
        remote(to_back.at[:, :split], from_back.at[:, :split], b_send.at[1], b_recv.at[1], to_x),
        remote(to_back.at[:, split:], from_back.at[:, split:], b_send.at[2], b_recv.at[2], to_x),
    ]

    def send_back(which, copies):
        for i in which:
            to_back[:, corner_row[i]:corner_row[i + 1]] = finish(corner[i]).astype(jnp.bfloat16)
        for copy in copies:
            copy.start()

    def write(member, total_of):
        at = pl.ds(pl.multiple_of(member * quarter, quarter), quarter)
        for t in range(targets):
            out[t, :, at] = parent[t, :, at] - total_of(t)

    def near_x(t):
        return jnp.concatenate(
            [summed[unit_of["near", k]][t, :sizes[k]] for k in range(len(sizes))], axis=0
        ).T

    def near_y(t):
        return jnp.concatenate(
            [summed[unit_of["near", k]][t, sizes[k]:] for k in reversed(range(len(sizes)))], axis=0
        ).T

    def diagonal(t):
        ties = [from_back[t, half:].astype(jnp.float32)]
        newest = from_home[0, t].astype(jnp.float32)
        for h in range(1, chips):
            newest = newest + from_home[h, t].astype(jnp.float32)
        ties.append(newest)
        falling = [newest] + [
            from_back[t, corner_row[i]:corner_row[i + 1]].astype(jnp.float32)
            for i in reversed(range(len(corner)))
        ]
        turned = jnp.concatenate(falling, axis=0)
        upper = turned.T[:half]
        tied = jnp.concatenate(ties, axis=0)
        crossed = from_back_y[t].astype(jnp.float32)
        lower = jnp.concatenate([crossed[:, half:], tied[:, half:]], axis=1)
        return jnp.concatenate([upper, lower], axis=0)

    def arrive(k):
        x_copy[k].wait_recv()
        y_copy[k].wait_recv()

    make(u_own)
    meet_line()
    pass_on(u_own)
    relay(u_own)
    load_parent.wait()
    for k in range(len(sizes)):
        new = [unit_of[kind, k] for kind in ("tie", "near", "cross") if (kind, k) in unit_of]
        arrive(k)
        if k < last:
            for u in new:
                make(u)
        else:
            for f in range(fronts):
                if f:
                    arrive(k + f)
                for u in new:
                    multiply(u, slice(f, f + 1))
                    if f == fronts - 1:
                        add_up(u)
        for u in new:
            pass_on(u)
        if k == middle:
            for group, u in enumerate(early):
                arrived(group)
                settle(u)
            write(g, lambda t: summed[u_own][t].T)
        for u in new:
            if u in relayed:
                relay(u)
    arrived(2)
    arrived(3)
    send_back(range(len(corner) - 1), back[:2])
    for k in range(1, last - 1):
        settle(unit_of["near", k])
    arrived(4)
    send_back([len(corner) - 1], back[2:])
    settle(unit_of["near", last - 1])
    arrived(5)
    settle(unit_of["near", last])
    write(x_peer, near_x)
    write(y_peer, near_y)
    for copy in back:
        copy.wait_recv()
    whole_home = remote(to_home, from_home, h_send.at[0], h_recv.at[0], to_x)
    whole_home.wait_recv()
    write(d_peer, diagonal)
    for copy in back + [
        whole_home,
        remote(own, from_x, x_send.at[0], x_recv.at[0], to_x),
        remote(own, from_y, y_send.at[0], y_recv.at[0], to_y),
        *p_copy.values(),
        remote(to_chip, to_chip, z_send.at[0], z_recv.at[0], to_beside),
    ]:
        copy.wait_send()


def fused(panels, parent, src_block, dest_owner, target, counts, chips, capacity):
    fronts, blocks, quarter, width = panels.shape
    targets = parent.shape[0]
    pairs = blocks * (blocks + 1) // 2
    sizes, _, middle, units = plan(quarter)
    heights = [high for _, _, high in units]
    relayed, direct, _, _, (relay_rows, direct_rows) = layout(units, middle)
    tie = units[-2][2]
    corner_rows = sum(high for kind, _, high in units if kind in ("cross", "tie")) - tie

    def buffer(count, rows):
        return pltpu.VMEM((count, targets, rows, quarter), jnp.bfloat16)

    def sums(lead):
        return [pltpu.VMEM(lead + (targets, high, quarter), jnp.float32) for high in heights]

    def back(rows):
        return pltpu.VMEM((targets, rows, quarter), jnp.bfloat16)

    whole = pltpu.VMEM((fronts, blocks, quarter, width), panels.dtype)
    dma = pltpu.SemaphoreType.DMA
    slots = pltpu.SMEM(src_block.shape, jnp.int32)
    arrays = pl.BlockSpec(memory_space=pltpu.VMEM)
    there = pl.BlockSpec(memory_space=pl.ANY)
    home = buffer(chips, tie)
    return pl.pallas_call(
        functools.partial(kernel, chips, capacity),
        out_shape=pltpu.VMEM(parent.shape, parent.dtype),
        in_specs=[there] * 6,
        out_specs=arrays,
        scratch_shapes=[
            slots, slots, slots, pltpu.SMEM((1, 1), jnp.int32),
            pltpu.SMEM((2, 2 * chips * capacity), jnp.int32),
            whole, pltpu.VMEM(parent.shape, parent.dtype), whole, whole,
            pltpu.VMEM((fronts * pairs, quarter, quarter), jnp.bfloat16),
            pltpu.VMEM((fronts * pairs, quarter // 4, quarter), jnp.bfloat16),
            sums((chips,)), sums(()),
            [buffer(chips, high) for high in heights], [buffer(chips, high) for high in heights],
            buffer(chips - 1, relay_rows + direct_rows), buffer(chips - 2, relay_rows),
            buffer(chips - 1, direct_rows), buffer(chips - 2, relay_rows),
            back(corner_rows), back(corner_rows), back(quarter // 2), home, home,
            dma((1,)), dma((len(sizes) + fronts,)), dma((1,)), dma((len(sizes) + fronts,)),
            dma((len(units),)), dma((len(units),)), dma((1,)), dma((6,)), dma((len(relayed), chips - 2)),
            dma((3,)), dma((3,)),
            pltpu.SemaphoreType.REGULAR((2,)), dma((1,)), dma((1,)), dma((9,)),
        ],
        compiler_params=pltpu.CompilerParams(
            collective_id=0, has_side_effects=True, vmem_limit_bytes=60 * 1024 * 1024
        ),
    )(src_block, dest_owner.reshape(1, -1), target.reshape(1, -1), counts.reshape(1, 1), panels, parent)


def per_device(panels, parent, src_block, dest_owner, target, counts):
    fronts, blocks, quarter, _ = panels.shape
    pair_count = blocks * (blocks + 1) // 2
    peer_count = lax.axis_size("col")
    slot_count = src_block.shape[1]
    capacity = (slot_count + peer_count - 1) // peer_count + slot_count // (2 * peer_count)
    targets = parent.shape[0]
    if lax.axis_size("grp") == 4 and peer_count == 8 and targets < capacity and quarter == 128:
        return fused(
            panels, parent, src_block, dest_owner, target, counts, peer_count // 2, capacity
        )
    chosen, position, is_live, routed = place_slots(
        src_block, dest_owner, target, counts, peer_count, capacity
    )
    products = pair_products(panels, lax.all_gather(panels, "grp", axis=2, tiled=True))
    flat_updates = products.reshape(fronts * pair_count, quarter, products.shape[3])
    buffer = pack_updates(flat_updates, chosen, position, is_live, peer_count, capacity)
    received, labels = (
        lax.all_to_all(buffer, "col", split_axis=0, concat_axis=0, tiled=True),
        lax.all_to_all(routed, "col", split_axis=0, concat_axis=0, tiled=True),
    )
    return parent - assemble(received, labels, targets)


def solution(mesh):
    placed = (
        P("col", None, "grp", None),
        P("col", "grp", None),
        P("col", None),
        P("col", None),
        P("col"),
        P("col"),
    )
    return jax.shard_map(
        per_device, mesh=mesh, in_specs=placed, out_specs=P("col", "grp", None), check_vma=False
    )
```

```python
import functools

import jax
import jax.numpy as jnp
import numpy as np
from jax import lax
from jax.experimental import pallas as pl
from jax.experimental.pallas import tpu as pltpu
from jax.sharding import PartitionSpec as P

MESH = pl.DeviceIdType.MESH


def place_slots(src_block, dest_owner, target, counts, peer_count, capacity):
    slot_count = src_block.shape[1]
    slot_index = jnp.arange(slot_count, dtype=jnp.int32)
    owner_rank = dest_owner[:, 0]
    matches = (owner_rank[:, None] == jnp.arange(peer_count, dtype=jnp.int32)[None, :]).astype(
        jnp.int32
    )
    earlier = jnp.cumsum(matches, axis=0) - matches
    rank_in = jnp.sum(earlier * matches, axis=1)
    position = owner_rank * capacity + rank_in
    is_live = slot_index < counts[0]
    routed = jnp.zeros((peer_count * capacity,), jnp.int32).at[position].set(target)
    return (src_block[0], position, is_live, routed.reshape(peer_count, capacity))


def pack_updates(flat_updates, chosen, position, is_live, peer_count, capacity):
    picked = flat_updates[chosen]
    picked = jnp.where(is_live[:, None, None], picked, jnp.zeros_like(picked))
    buffer = (
        jnp.zeros((peer_count * capacity,) + picked.shape[1:], picked.dtype)
        .at[position]
        .set(picked)
    )
    return buffer.reshape((peer_count, capacity) + picked.shape[1:])


def assemble(received, labels, targets):
    arrived = received.reshape((-1,) + received.shape[2:])
    flat_labels = labels.reshape(-1)
    select = (flat_labels[None, :] == jnp.arange(targets, dtype=jnp.int32)[:, None]).astype(
        jnp.bfloat16
    )
    return jnp.einsum("tn,nrc->trc", select, arrived, preferred_element_type=jnp.float32)


def pair_products(own_rows, piece_rows):
    blocks = own_rows.shape[1]
    upper_table = np.array([a for a in range(blocks) for b in range(a + 1)], np.int32)
    lower_table = np.array([b for a in range(blocks) for b in range(a + 1)], np.int32)
    left_rows = own_rows[:, upper_table]
    right_rows = piece_rows[:, lower_table]
    return jnp.einsum(
        "fprw,fpcw->fprc", left_rows, right_rows, preferred_element_type=jnp.float32
    ).astype(jnp.bfloat16)


def plan(quarter):
    sizes = [quarter // 4] + [quarter // 8] * 6
    ends = [sum(sizes[: k + 1]) for k in range(len(sizes))]
    middle = ends.index(quarter // 2)
    units = [("own", -1, quarter)]
    for k, size in enumerate(sizes):
        if k == middle:
            units.append(("cross", k, quarter // 2))
        if k > middle:
            units.append(("tie", k, size))
        units.append(("near", k, 2 * size))
    return sizes, ends, middle, units


def layout(units, middle):
    relayed, direct = [], []
    for u, (kind, k, _) in enumerate(units):
        (relayed if k <= middle - 1 else direct).append(u)
    home = direct[-2]
    direct = [u for u in direct if u != home]
    first = {}
    counts = []
    for group in (relayed, direct):
        row = 0
        for u in group:
            first[u] = row
            row += units[u][2]
        counts.append(row)
    return relayed, direct, home, first, counts


def kernel(
    chips, capacity, src_block_in, owner_in, target_in, counts_in, panels, parent_in, out,
    src_block, owner, target, counts, table, own, parent, from_x, from_y, product, tie_product, kept, summed, to_pair, from_pair,
    to_chip, from_relay, from_direct, cargo, to_back, from_back, from_back_y, to_home, from_home,
    x_send, x_recv, y_send, y_recv, p_send, p_recv, z_send, z_recv, c_recv, b_send, b_recv,
    ready, h_send, h_recv, l_sem,
):
    fronts, blocks, quarter, width = own.shape
    share = quarter // 4
    load_own = [
        pltpu.make_async_copy(
            panels.at[:, :, pl.ds(i * share, share)], own.at[:, :, pl.ds(i * share, share)],
            l_sem.at[1 + i],
        )
        for i in range(4)
    ]
    load_parent = pltpu.make_async_copy(parent_in, parent, l_sem.at[0])
    for i in (0, 3, 1, 2):
        load_own[i].start()
    load_slots = [
        pltpu.make_async_copy(given, kept_at, l_sem.at[5 + i])
        for i, (given, kept_at) in enumerate((
            (src_block_in, src_block), (owner_in, owner), (target_in, target), (counts_in, counts)
        ))
    ]
    for copy in load_slots:
        copy.start()
    targets = parent.shape[0]
    pairs = blocks * (blocks + 1) // 2
    slots = src_block.shape[1]
    half = quarter // 2
    sizes, ends, middle, units = plan(quarter)
    last = len(sizes) - 1
    relayed, direct, u_home, first_row, (relay_rows, direct_rows) = layout(units, middle)
    unit_of = {(kind, k): u for u, (kind, k, _) in enumerate(units)}
    g, c = lax.axis_index("grp"), lax.axis_index("col")
    gy, gx = g // 2, g % 2
    z, core = c // 2, c % 2
    x_peer = gy * 2 + (1 - gx)
    y_peer = (1 - gy) * 2 + gx
    d_peer = 3 - g
    to_x, to_y = {"grp": x_peer, "col": c}, {"grp": y_peer, "col": c}
    to_core = {"grp": g, "col": z * 2 + 1 - core}
    far = [lax.rem(z + hop, chips) for hop in range(1, chips)]
    to_far = [{"grp": g, "col": chip * 2 + core} for chip in far]
    edge = jnp.logical_or(z == 0, z == chips - 1)
    beside = z + 1 - 2 * (z % 2)
    inner = jnp.where(z < 2, 2, 1)
    outer = jnp.where(z < 2, 3, 0)
    to_beside, to_inner, to_outer = (
        {"grp": g, "col": chip * 2 + core} for chip in (beside, inner, outer)
    )
    homes = far + [z]
    to_homes = [{"grp": x_peer, "col": chip * 2 + core} for chip in homes]

    barrier = pltpu.get_barrier_semaphore()

    def greet(semaphore, peers):
        for peer in peers:
            pl.semaphore_signal(semaphore, inc=1, device_id=peer, device_id_type=MESH)

    plane = [{"grp": peer, "col": z * 2} for peer in (x_peer, y_peer)]
    greet(barrier, plane)

    @pl.when(core == 1)
    def _():
        greet(barrier, [to_core])

    @pl.when(core == 0)
    def _():
        pl.semaphore_wait(barrier, 5)
        greet(ready.at[0], [to_core])

    @pl.when(core == 1)
    def _():
        pl.semaphore_wait(ready.at[0], 1)

    def meet_line():
        @pl.when(core == 1)
        def _():
            pl.semaphore_wait(barrier, 2 * (chips - 1))
            greet(ready.at[1], [to_core])

        @pl.when(core == 0)
        def _():
            pl.semaphore_wait(ready.at[1], 1)

    def remote(src, dst, send, recv, device):
        return pltpu.make_async_remote_copy(
            src_ref=src, dst_ref=dst, send_sem=send, recv_sem=recv,
            device_id=device, device_id_type=MESH,
        )

    def x_rows(k):
        return slice(ends[k] - sizes[k], ends[k])

    def y_rows(k):
        return slice(quarter - ends[k], quarter - ends[k] + sizes[k])

    def static(rows):
        return pl.ds(rows.start, rows.stop - rows.start)

    def panel_copies(rows_of, into, send, recv, to):
        copies = []
        for k in range(len(sizes)):
            rows = static(rows_of(k))
            parts = [slice(0, fronts)] if k < last else [slice(f, f + 1) for f in range(fronts)]
            for part in parts:
                at = (static(part), slice(None), rows)
                copies.append(
                    remote(own.at[at], into.at[at], send.at[0], recv.at[len(copies)], to)
                )
        return copies

    x_copy = panel_copies(x_rows, from_x, x_send, x_recv, to_x)
    y_copy = panel_copies(y_rows, from_y, y_send, y_recv, to_y)
    load_own[0].wait()
    x_copy[0].start()
    load_own[3].wait()
    y_copy[0].start()
    load_own[1].wait()
    load_own[2].wait()
    load_parent.start()
    for i in range(1, len(x_copy)):
        x_copy[i].start()
        y_copy[i].start()

    @pl.when(core == 1)
    def _():
        greet(barrier, to_far + to_homes[:-1])

    bits = (fronts * pairs * 8 - 1).bit_length()
    per_word = 31 // bits
    words = -(-capacity // per_word)
    mask = (1 << (bits * per_word)) - 1

    def list_owners(first, count):
        def look(s, state):
            value = src_block[0, s] * 8 + jnp.where(s < counts[0, 0], target[0, s] + 1, 0)
            named = owner[0, s]
            after = []
            for i in range(count):
                mine = named == first + i
                held = state[i * words:(i + 1) * words]
                carry = value
                for word in held:
                    moved = ((word << bits) & mask) | carry
                    carry = word >> (bits * (per_word - 1))
                    after.append(jnp.where(mine, moved, word))
            return tuple(after)

        state = lax.fori_loop(0, slots, look, (jnp.int32(0),) * (words * count))
        for i in range(count):
            for k in range(capacity):
                word = state[i * words + k // per_word]
                item = (word >> (bits * (k % per_word))) & ((1 << bits) - 1)
                table[0, (first + i) * capacity + k] = item >> 3
                table[1, (first + i) * capacity + k] = item & 7

    for copy in load_slots:
        copy.wait()
    for first in range(0, 2 * chips, 4):
        list_owners(first, min(4, 2 * chips - first))

    def rows_in(u):
        return pl.ds(first_row[u], units[u][2])

    def rows_all(u):
        if u == u_home:
            return pl.ds(relay_rows + direct_rows, units[u][2])
        return pl.ds(first_row[u] + (0 if u in relayed else relay_rows), units[u][2])

    early = relayed[:2]
    z_group = {u: early.index(u) if u in early else 2 for u in relayed}
    z_group.update({u: 3 + max(0, units[u][1] - last + 2) for u in direct})

    def blocks_out(u):
        if u in relayed:
            to, slots_at, into = [to_beside, to_inner, to_outer], [0, 1, 1], from_relay
        else:
            to, slots_at, into = to_far, [0, 1, 2], from_direct
        return [
            remote(
                to_chip.at[h, :, rows_all(u)], into.at[slots_at[h], :, rows_in(u)],
                z_send.at[0], z_recv.at[z_group[u]], to[h],
            )
            for h in range(chips - 1)
        ]

    p_copy, z_copy, c_copy = {}, {}, {}
    for u in range(len(units)):
        p_copy[u] = remote(to_pair[u], from_pair[u], p_send.at[u], p_recv.at[u], to_core)
        if u != u_home:
            z_copy[u] = blocks_out(u)
    for i, u in enumerate(relayed):
        c_copy[u] = [
            remote(
                to_chip.at[h, :, rows_all(u)], cargo.at[h - 1, :, rows_in(u)],
                z_send.at[0], c_recv.at[i, h - 1], to_beside,
            )
            for h in range(1, chips - 1)
        ]
    h_copy = [
        remote(to_home.at[h], from_home.at[h], h_send.at[0], h_recv.at[0], to_homes[h])
        for h in range(chips)
    ]

    def select(made, high, parity, store):
        tile = min(32, high)

        def chip(zz, carry):
            base = (zz * 2 + parity) * capacity
            chosen = [table[0, base + k] for k in range(capacity)]
            label = [table[1, base + k] for k in range(capacity)]
            weight = [
                [jnp.where(label[k] == t + 1, 1.0, 0.0).astype(jnp.float32) for t in range(targets)]
                for k in range(capacity)
            ]

            def rows(i, carry):
                start = pl.multiple_of(i * tile, tile)
                taken = [
                    made[chosen[k], pl.ds(start, tile), :].astype(jnp.float32)
                    for k in range(capacity)
                ]
                for t in range(targets):
                    total = taken[0] * weight[0][t]
                    for k in range(1, capacity):
                        total = total + taken[k] * weight[k][t]
                    store(zz, t, start, tile, total)
                return carry

            return lax.fori_loop(0, high // tile, rows, carry, unroll=True)

        lax.fori_loop(0, chips, chip, 0, unroll=True)

    def dot(left, right):
        return lax.dot_general(
            left, right, (((1,), (1,)), ((), ())), preferred_element_type=jnp.float32
        ).astype(jnp.bfloat16)

    def stack(f, parts):
        return [jnp.concatenate([ref[f, b, rows] for ref, rows in parts], axis=0) for b in range(blocks)]

    every = slice(0, quarter)

    def against_own(f, parts, high):
        left = stack(f, parts)
        for first in range(0, blocks, 2):
            width_of = min(2, blocks - first)
            right = jnp.concatenate([own[f, first + i] for i in range(width_of)], axis=0)
            made = dot(jnp.concatenate(left[:first + width_of], axis=0), right)
            for i in range(width_of):
                a = first + i
                for b in range(a + 1):
                    product[f * pairs + a * (a + 1) // 2 + b, :high] = made[
                        b * high:(b + 1) * high, i * quarter:(i + 1) * quarter
                    ]

    def grid(f, left, left_rows, right, right_rows):
        return dot(
            jnp.concatenate(stack(f, [(left, left_rows)]), axis=0),
            jnp.concatenate(stack(f, [(right, right_rows)]), axis=0),
        )

    def paired(into, f, high, lower, upper):
        for a in range(blocks):
            for b in range(a + 1):
                into[f * pairs + a * (a + 1) // 2 + b, :high] = jnp.concatenate(
                    [lower(a, b), upper(a, b)], axis=1
                )

    def product_of(u):
        return tie_product if units[u][0] == "tie" else product

    def multiply(u, some):
        kind, k, high = units[u]

        def front(f, carry):
            if kind == "own":
                against_own(f, [(own, every)], high)
            elif kind == "near":
                against_own(f, [(from_x, x_rows(k)), (from_y, y_rows(k))], high)
            elif kind == "cross":
                made = grid(f, from_y, slice(half, quarter), from_x, slice(0, half))

                def piece(p, q):
                    return made[p * high:(p + 1) * high, q * half:(q + 1) * half]

                paired(product, f, high, lambda a, b: piece(b, a), lambda a, b: piece(a, b))
            else:
                by_y = grid(f, from_y, y_rows(k), from_x, slice(0, half))
                by_x = grid(f, from_x, x_rows(k), from_y, slice(half, quarter))

                def piece(made, p, q):
                    return made[p * high:(p + 1) * high, q * half:(q + 1) * half]

                paired(
                    tie_product, f, high, lambda a, b: piece(by_y, b, a), lambda a, b: piece(by_x, a, b)
                )
            return carry

        if some == slice(0, fronts):
            lax.fori_loop(0, fronts, front, 0, unroll=True)
        else:
            for f in range(some.start, some.stop):
                front(f, 0)

    def add_up(u):
        high = units[u][2]

        def store_pair(zz, t, start, tile, total):
            to_pair[u][zz, t, pl.ds(start, tile), :] = total.astype(jnp.bfloat16)

        def store_kept(zz, t, start, tile, total):
            kept[u][zz, t, pl.ds(start, tile), :] = total

        def give():
            select(product_of(u), high, 1 - core, store_pair)
            p_copy[u].start()

        def keep():
            select(product_of(u), high, core, store_kept)

        return give, keep

    def make(u):
        multiply(u, slice(0, fronts))
        for part in add_up(u):
            part()

    def paired_sum(u, chip):
        return kept[u][chip] + from_pair[u][chip].astype(jnp.float32)

    def pass_on(u):
        p_copy[u].wait_recv()
        if u == u_home:
            for h in range(chips):
                to_home[h] = paired_sum(u, homes[h]).astype(jnp.bfloat16)
                h_copy[h].start()
            return
        at = rows_all(u)
        if u not in relayed:
            for h in range(chips - 1):
                to_chip[h, :, at] = paired_sum(u, far[h]).astype(jnp.bfloat16)
                z_copy[u][h].start()
        else:
            @pl.when(edge)
            def _():
                for h, chip in ((2, outer), (1, inner)):
                    to_chip[h, :, at] = paired_sum(u, chip).astype(jnp.bfloat16)
                    c_copy[u][h - 1].start()

            to_chip[0, :, at] = paired_sum(u, beside).astype(jnp.bfloat16)
            z_copy[u][0].start()
        summed[u][...] = paired_sum(u, z)

    def relay(u):
        @pl.when(jnp.logical_not(edge))
        def _():
            for h, chip in ((2, outer), (1, inner)):
                c_copy[u][h - 1].wait_recv()
                to_chip[h, :, rows_all(u)] = (
                    paired_sum(u, chip) + cargo[h - 1, :, rows_in(u)].astype(jnp.float32)
                ).astype(jnp.bfloat16)
                z_copy[u][h].start()

    def arrived(group):
        members = [u for u in z_group if z_group[u] == group]
        into, count = (from_relay, chips - 2) if members[0] in relayed else (from_direct, chips - 1)
        rows = pl.ds(first_row[members[0]], sum(units[u][2] for u in members))
        remote(
            to_chip.at[:count, :, rows], into.at[:, :, rows],
            z_send.at[0], z_recv.at[group], to_beside,
        ).wait_recv()

    def finish(u):
        into, count = (from_relay, chips - 2) if u in relayed else (from_direct, chips - 1)
        total = summed[u][...]
        for h in range(count):
            total = total + into[h, :, rows_in(u)].astype(jnp.float32)
        return total

    def settle(u):
        summed[u][...] = finish(u)

    u_own = unit_of["own", -1]
    corner = [unit_of["cross", middle]] + [unit_of["tie", k] for k in range(middle + 1, last)]
    corner_row = [sum(units[v][2] for v in corner[:i]) for i in range(len(corner) + 1)]
    split = corner_row[-2]
    back = [
        remote(to_back.at[:, :half], from_back_y, b_send.at[0], b_recv.at[0], to_y),
        remote(to_back.at[:, :split], from_back.at[:, :split], b_send.at[1], b_recv.at[1], to_x),
        remote(to_back.at[:, split:], from_back.at[:, split:], b_send.at[2], b_recv.at[2], to_x),
    ]

    def send_back(which, copies):
        for i in which:
            to_back[:, corner_row[i]:corner_row[i + 1]] = finish(corner[i]).astype(jnp.bfloat16)
        for copy in copies:
            copy.start()

    def write(member, total_of):
        at = pl.ds(pl.multiple_of(member * quarter, quarter), quarter)
        for t in range(targets):
            out[t, :, at] = parent[t, :, at] - total_of(t)

    def near_x(t):
        return jnp.concatenate(
            [summed[unit_of["near", k]][t, :sizes[k]] for k in range(len(sizes))], axis=0
        ).T

    def near_y(t):
        return jnp.concatenate(
            [summed[unit_of["near", k]][t, sizes[k]:] for k in reversed(range(len(sizes)))], axis=0
        ).T

    def diagonal(t):
        ties = [from_back[t, half:].astype(jnp.float32)]
        newest = from_home[0, t].astype(jnp.float32)
        for h in range(1, chips):
            newest = newest + from_home[h, t].astype(jnp.float32)
        ties.append(newest)
        falling = [newest] + [
            from_back[t, corner_row[i]:corner_row[i + 1]].astype(jnp.float32)
            for i in reversed(range(len(corner)))
        ]
        turned = jnp.concatenate(falling, axis=0)
        upper = turned.T[:half]
        tied = jnp.concatenate(ties, axis=0)
        crossed = from_back_y[t].astype(jnp.float32)
        lower = jnp.concatenate([crossed[:, half:], tied[:, half:]], axis=1)
        return jnp.concatenate([upper, lower], axis=0)

    def arrive(k):
        x_copy[k].wait_recv()
        y_copy[k].wait_recv()

    make(u_own)
    meet_line()
    pass_on(u_own)
    relay(u_own)
    load_parent.wait()
    for k in range(len(sizes)):
        new = [unit_of[kind, k] for kind in ("tie", "near", "cross") if (kind, k) in unit_of]
        arrive(k)
        if k < last:
            for u in new:
                make(u)
        else:
            for f in range(fronts):
                if f:
                    arrive(k + f)
                for u in new:
                    multiply(u, slice(f, f + 1))
                    if f == fronts - 1:
                        add_up(u)[0]()
            for u in new:
                add_up(u)[1]()
        for u in new:
            pass_on(u)
        if k == middle:
            for group, u in enumerate(early):
                arrived(group)
                settle(u)
            write(g, lambda t: summed[u_own][t].T)
        for u in new:
            if u in relayed:
                relay(u)
    arrived(2)
    arrived(3)
    send_back(range(len(corner) - 1), back[:2])
    for k in range(1, last - 1):
        settle(unit_of["near", k])
    arrived(4)
    send_back([len(corner) - 1], back[2:])
    settle(unit_of["near", last - 1])
    arrived(5)
    settle(unit_of["near", last])
    write(x_peer, near_x)
    write(y_peer, near_y)
    for copy in back:
        copy.wait_recv()
    whole_home = remote(to_home, from_home, h_send.at[0], h_recv.at[0], to_x)
    whole_home.wait_recv()
    write(d_peer, diagonal)
    for copy in back + [
        whole_home,
        remote(own, from_x, x_send.at[0], x_recv.at[0], to_x),
        remote(own, from_y, y_send.at[0], y_recv.at[0], to_y),
        *p_copy.values(),
        remote(to_chip, to_chip, z_send.at[0], z_recv.at[0], to_beside),
    ]:
        copy.wait_send()


def fused(panels, parent, src_block, dest_owner, target, counts, chips, capacity):
    fronts, blocks, quarter, width = panels.shape
    targets = parent.shape[0]
    pairs = blocks * (blocks + 1) // 2
    sizes, _, middle, units = plan(quarter)
    heights = [high for _, _, high in units]
    relayed, direct, _, _, (relay_rows, direct_rows) = layout(units, middle)
    tie = units[-2][2]
    corner_rows = sum(high for kind, _, high in units if kind in ("cross", "tie")) - tie

    def buffer(count, rows):
        return pltpu.VMEM((count, targets, rows, quarter), jnp.bfloat16)

    def sums(lead):
        return [pltpu.VMEM(lead + (targets, high, quarter), jnp.float32) for high in heights]

    def back(rows):
        return pltpu.VMEM((targets, rows, quarter), jnp.bfloat16)

    whole = pltpu.VMEM((fronts, blocks, quarter, width), panels.dtype)
    dma = pltpu.SemaphoreType.DMA
    slots = pltpu.SMEM(src_block.shape, jnp.int32)
    arrays = pl.BlockSpec(memory_space=pltpu.VMEM)
    there = pl.BlockSpec(memory_space=pl.ANY)
    home = buffer(chips, tie)
    return pl.pallas_call(
        functools.partial(kernel, chips, capacity),
        out_shape=pltpu.VMEM(parent.shape, parent.dtype),
        in_specs=[there] * 6,
        out_specs=arrays,
        scratch_shapes=[
            slots, slots, slots, pltpu.SMEM((1, 1), jnp.int32),
            pltpu.SMEM((2, 2 * chips * capacity), jnp.int32),
            whole, pltpu.VMEM(parent.shape, parent.dtype), whole, whole,
            pltpu.VMEM((fronts * pairs, quarter, quarter), jnp.bfloat16),
            pltpu.VMEM((fronts * pairs, quarter // 4, quarter), jnp.bfloat16),
            sums((chips,)), sums(()),
            [buffer(chips, high) for high in heights], [buffer(chips, high) for high in heights],
            buffer(chips - 1, relay_rows + direct_rows), buffer(chips - 2, relay_rows),
            buffer(chips - 1, direct_rows), buffer(chips - 2, relay_rows),
            back(corner_rows), back(corner_rows), back(quarter // 2), home, home,
            dma((1,)), dma((len(sizes) + fronts,)), dma((1,)), dma((len(sizes) + fronts,)),
            dma((len(units),)), dma((len(units),)), dma((1,)), dma((6,)), dma((len(relayed), chips - 2)),
            dma((3,)), dma((3,)),
            pltpu.SemaphoreType.REGULAR((2,)), dma((1,)), dma((1,)), dma((9,)),
        ],
        compiler_params=pltpu.CompilerParams(
            collective_id=0, has_side_effects=True, vmem_limit_bytes=60 * 1024 * 1024
        ),
    )(src_block, dest_owner.reshape(1, -1), target.reshape(1, -1), counts.reshape(1, 1), panels, parent)


def per_device(panels, parent, src_block, dest_owner, target, counts):
    fronts, blocks, quarter, _ = panels.shape
    pair_count = blocks * (blocks + 1) // 2
    peer_count = lax.axis_size("col")
    slot_count = src_block.shape[1]
    capacity = (slot_count + peer_count - 1) // peer_count + slot_count // (2 * peer_count)
    targets = parent.shape[0]
    if lax.axis_size("grp") == 4 and peer_count == 8 and targets < capacity and quarter == 128:
        return fused(
            panels, parent, src_block, dest_owner, target, counts, peer_count // 2, capacity
        )
    chosen, position, is_live, routed = place_slots(
        src_block, dest_owner, target, counts, peer_count, capacity
    )
    products = pair_products(panels, lax.all_gather(panels, "grp", axis=2, tiled=True))
    flat_updates = products.reshape(fronts * pair_count, quarter, products.shape[3])
    buffer = pack_updates(flat_updates, chosen, position, is_live, peer_count, capacity)
    received, labels = (
        lax.all_to_all(buffer, "col", split_axis=0, concat_axis=0, tiled=True),
        lax.all_to_all(routed, "col", split_axis=0, concat_axis=0, tiled=True),
    )
    return parent - assemble(received, labels, targets)


def solution(mesh):
    placed = (
        P("col", None, "grp", None),
        P("col", "grp", None),
        P("col", None),
        P("col", None),
        P("col"),
        P("col"),
    )
    return jax.shard_map(
        per_device, mesh=mesh, in_specs=placed, out_specs=P("col", "grp", None), check_vma=False
    )
```
